128 devices in a mesh: blk: 32 (over y_lo, x, z), ga: 4 (over y_hi, core).
Axes of the slice: x: 4, y: 4 (y_hi: 2, y_lo: 2; y = y_hi * 2 + y_lo), z: 4, core: 2. Of those that a mesh axis runs over, the one named last changes fastest.
Arguments:
- pair_val: bfloat16 [64, 64, 16, 2048], P('blk', None, None, 'ga'), may hold values from -0.125 to 0.125
- pair_con: bfloat16 [64, 64, 16, 2048], P('blk', None, None, 'ga'), may hold values from -6 to 6
- screened: bfloat16 [64, 2048, 2048], P('blk', None, 'ga'), may hold values from -0.125 to 0.125
- amplitude: bfloat16 [64, 16], P('blk'), may hold values from -6 to 6
- qmap: int32 [64, 64], P('blk'), may hold values from 0 to 63, as said below
Outputs:
- kernel_x: float32 [64, 16], P('blk')
The draws below stay inside these ranges and needn't reach their ends.
Inputs may be any that keep to these rules, and one draw needn't show every extreme that they name: qmap[k, k'] is the label of the difference k - k' (periodic) on a grid of 8 by 8 points, with the points and the differences labelled at random; every row and every column holds each label once.
All inputs are finite; a program needn't handle non-finite values.
Results may differ from the reference program's by a relative error of at most 0.004.
Values may be sent and summed in bfloat16 or wider, within the bound.
A program may use at most 64 MiB of HBM per device.

```python
import jax
import jax.numpy as jnp
from jax import lax

NV = 4
NC = 4
NG = 2048
GRID_X = 8
NK = 64


def draw_qmap(key, part):
    point_order = jax.random.permutation(jax.random.fold_in(key, 11), NK)
    label_order = jax.random.permutation(jax.random.fold_in(key, 23), NK)
    rows_y = NK // GRID_X
    coord_x = point_order % GRID_X
    coord_y = point_order // GRID_X
    diff_x = (coord_x[:, None] - coord_x[None, :]) % GRID_X
    diff_y = (coord_y[:, None] - coord_y[None, :]) % rows_y
    return label_order[diff_y * GRID_X + diff_x].astype(jnp.int32)


def block_scale(own_key, shape, shards, smallest, high):
    factor_of, own = 1.0, jax.random.fold_in(own_key, 6)
    for dim, shards_of in shards:
        steps = jnp.exp(jax.random.uniform(jax.random.fold_in(own, dim), (shards_of,), jnp.float32, smallest / len(shards), high / len(shards)))
        factor_of = factor_of * jnp.repeat(steps, shape[dim] // shards_of).reshape([-1 if axis == dim else 1 for axis in range(len(shape))])
    return factor_of


def bell_draw(stream_key, shape, width, reach, pieces=(), held_as=jnp.bfloat16):
    values = width * jax.random.normal(stream_key, shape, jnp.float32)
    if pieces:
        values = values * block_scale(stream_key, shape, pieces, -0.22, 0.18)
    return jnp.clip(values, -reach, reach).astype(held_as)


def setup_inputs(seed: int = 0) -> dict:
    key_list = jax.random.split(jax.random.key(seed), 6)
    return {
        "pair_val": bell_draw(key_list[0], (NK, NK, NV * NV, NG), NG ** -0.5, 0.125, ((0, 32), (3, 4))),
        "pair_con": bell_draw(key_list[1], (NK, NK, NC * NC, NG), 1.0, 6.0, ((0, 32), (3, 4))),
        "screened": bell_draw(key_list[2], (NK, NG, NG), NG ** -0.5, 0.125, ((0, 32), (2, 4))),
        "amplitude": bell_draw(key_list[3], (NK, NV * NC), 1.0, 6.0, ((0, 32),)),
        "qmap": draw_qmap(jax.random.fold_in(key_list[5], 71), 0),
    }


def inverse_rows(qmap):
    total = qmap.shape[1]
    labels = jnp.arange(total, dtype=jnp.int32)
    hits = (qmap[:, :, None] == labels[None, None, :]).astype(jnp.int32)
    return jnp.sum(hits * labels[None, :, None], axis=1).astype(jnp.int32)


def reference(pair_val, pair_con, screened, amplitude, qmap):
    total = qmap.shape[0]
    partner = inverse_rows(qmap)
    rows = jnp.arange(total, dtype=jnp.int32)

    def per_label(label):
        chosen = lax.dynamic_index_in_dim(partner, label, 1, keepdims=False).astype(jnp.int32)
        values = pair_val[rows, chosen].astype(jnp.float32).reshape(total, NV, NV, NG)
        cons = pair_con[rows, chosen]
        amps = amplitude[chosen].astype(jnp.float32).reshape(total, NV, NC)
        zeta = jnp.einsum('navg,nvc->nacg', values, amps).astype(jnp.bfloat16)
        zeta = lax.optimization_barrier(zeta).astype(jnp.float32)
        weights = lax.dynamic_index_in_dim(screened, label, 0, keepdims=False)
        unit = jnp.dot(cons.reshape(total * NC * NC, NG), weights, preferred_element_type=jnp.float32).astype(jnp.bfloat16)
        unit = lax.optimization_barrier(unit).astype(jnp.float32).reshape(total, NC, NC, NG)
        return jnp.einsum('ncyg,nayg->nac', unit, zeta).reshape(total, NV * NC)

    parts = lax.map(per_label, rows)
    return jnp.sum(parts, 0) / total
```

```python
import functools

import jax
import jax.numpy as jnp
from jax import lax
from jax.experimental import pallas as pl
from jax.experimental.pallas import tpu as pltpu
from jax.sharding import PartitionSpec as P

MESH = pl.DeviceIdType.MESH
ORDER = ((0, 0), (1, 0), (3, 0), (0, 1), (0, 3), (1, 1), (3, 3), (1, 3), (3, 1), (2, 0), (0, 2), (2, 1), (1, 2), (2, 3), (3, 2), (2, 2))
LAG = 2


def inverse_rows(qmap):
    total = qmap.shape[1]
    labels = jnp.arange(total, dtype=jnp.int32)
    hits = (qmap[:, :, None] == labels[None, None, :]).astype(jnp.int32)
    return jnp.sum(hits * labels[None, :, None], axis=1)


def iota(shape, dim):
    return lax.broadcasted_iota(jnp.int32, shape, dim)


def zero_one(cond):
    return jnp.where(cond, 1.0, 0.0).astype(jnp.bfloat16)


def kernel(
    partner, con_hbm, val_hbm, w_hbm, qa_ref, out_ref,
    con_raw, val_raw, w, s_send, d_send, val_send, con_all, val_all, transit,
    unit, acc, weight, qa_all, part, res, fin,
    load_sem, s_rs, d_rs, y_rs, p_rs, val_rs, qa_rs, res_rs, fin_rs,
    con_ss, val_ss, relay_ss, d2d_ss, qa_ss, res_ss, fin_ss,
):
    blk, ga = lax.axis_index("blk"), lax.axis_index("ga")
    lo, x, z = blk // 16, (blk // 4) % 4, blk % 4
    h, c = ga // 2, ga % 2

    def dev(dx, dz, flip_lo=0, flip_h=0, flip_c=0):
        to_lo = (lo + flip_lo) % 2
        to_h = (h + flip_h) % 2
        to_c = (c + flip_c) % 2
        return (to_lo * 16 + ((x + dx + 4) % 4) * 4 + (z + dz + 4) % 4, to_h * 2 + to_c)

    barrier = pltpu.get_barrier_semaphore()
    greeted = [dev(-dx, -dz, fl) for dx, dz in ORDER for fl in (0, 1) if (dx, dz, fl) != (0, 0, 0)]
    greeted += [dev(0, 0, 0, 1), dev(0, 0, 1, 1), dev(0, 0, 0, 0, 1), dev(0, 0, 0, 1, 1)]
    for other in greeted:
        pl.semaphore_signal(barrier, inc=1, device_id=other, device_id_type=MESH)

    loads = [
        pltpu.make_async_copy(con_hbm, con_raw, load_sem.at[0]),
        pltpu.make_async_copy(val_hbm, val_raw, load_sem.at[1]),
        pltpu.make_async_copy(w_hbm, w, load_sem.at[2]),
    ]
    for load in loads:
        load.start()

    def send(src, dst, ss, rs, to):
        copy = pltpu.make_async_remote_copy(src, dst, ss, rs, device_id=to, device_id_type=MESH)
        copy.start()
        return copy

    def arrived(dst, rs):
        pltpu.make_async_copy(dst, dst, rs).wait()

    def labels_of(dx, dz, fl):
        to, _ = dev(dx, dz, fl)
        return to * 2

    qa_all[blk] = qa_ref[...]
    loads[0].wait()
    for t, (dx, dz) in enumerate(ORDER):
        for fl in (0, 1):
            first = labels_of(dx, dz, fl)
            for q in (0, 1):
                for k in (0, 1):
                    tile = con_raw[k, partner[k, first + q]]
                    if fl == 0 and t == 0:
                        con_all[0, 0, 0, 0, q, k] = tile
                    elif fl == 0:
                        s_send[t, q, k] = tile
                    elif t == 0:
                        transit[0, q, k] = tile
                    else:
                        d_send[t, q, k] = tile
    pl.semaphore_wait(barrier, len(greeted))

    for t, (dx, dz) in enumerate(ORDER):
        if t:
            to = dev(dx, dz)
            send(d_send.at[t], transit.at[t], con_ss.at[0], d_rs.at[t], to)
            send(s_send.at[t], con_all.at[0, 0, t, 0], con_ss.at[1], s_rs.at[t], to)

    def relay(t):
        if t:
            arrived(transit.at[t], d_rs.at[t])
        send(transit.at[t], con_all.at[0, 0, t, 1], relay_ss.at[0], y_rs.at[0, t], dev(0, 0, 1))
        send(transit.at[t], con_all.at[0, 1, t, 1], relay_ss.at[1], y_rs.at[1, t], dev(0, 0, 1, 1))
        here = con_all.at[0, 0, t, 0]
        if t:
            arrived(here, s_rs.at[t])
        send(here, con_all.at[0, 1, t, 0], relay_ss.at[2], y_rs.at[2, t], dev(0, 0, 0, 1))
        send(here, con_all.at[1, 0, t, 0], d2d_ss.at[3], p_rs.at[3, t], dev(0, 0, 0, 0, 1))

    COLUMN = ((0, 1), (1, 1), (1, 0))

    def forward(t):
        for n, (gh, fl) in enumerate(COLUMN):
            arrived(con_all.at[0, gh, t, fl], y_rs.at[n, t])
            send(con_all.at[0, gh, t, fl], con_all.at[1, gh, t, fl], d2d_ss.at[n], p_rs.at[n, t], dev(0, 0, 0, 0, 1))

    relay(0)

    loads[1].wait()
    for t, (dx, dz) in enumerate(ORDER):
        for fl in (0, 1):
            first = labels_of(dx, dz, fl)
            for q in (0, 1):
                for k in (0, 1):
                    tile = val_raw[k, partner[k, first + q]]
                    if fl == 0 and t == 0:
                        val_all[0, q, k] = tile
                    else:
                        val_send[t * 2 + fl, q, k] = tile

    for t, (dx, dz) in enumerate(ORDER):
        for fl in (0, 1):
            if t or fl:
                send(qa_ref, qa_all.at[blk], qa_ss, qa_rs, dev(dx, dz, fl))
    for t, (dx, dz) in enumerate(ORDER):
        for fl in (1, 0):
            if t or fl:
                send(val_send.at[t * 2 + fl], val_all.at[t * 2 + fl], val_ss, val_rs.at[t * 2 + fl], dev(dx, dz, fl))

    def weights():
        arrived(qa_all.at[pl.ds(1, 31)], qa_rs)
        every = qa_all[...].reshape(64, 128)
        amps = every.astype(jnp.bfloat16)
        pick = zero_one(iota((128, 128), 0) == iota((128, 128), 1) + 64)
        amps = jnp.dot(amps, pick, preferred_element_type=jnp.float32).astype(jnp.bfloat16)
        row = iota((64, 64), 0)
        source = jnp.zeros((64, 64), jnp.int32)
        for t, (dx, dz) in enumerate(ORDER):
            for fl in (0, 1):
                source = jnp.where(row // 2 == t * 2 + fl, labels_of(-dx, -dz, fl), source)
        perm = zero_one(source + row % 2 == iota((64, 64), 1))
        for q in (0, 1):
            mine = (blk * 2 + q).astype(jnp.float32)
            hot = zero_one(every[:, :64] == mine)
            chosen = jnp.dot(hot, amps, preferred_element_type=jnp.float32).astype(jnp.bfloat16)
            chosen = jnp.dot(perm, chosen, preferred_element_type=jnp.float32).astype(jnp.bfloat16)
            spread = zero_one(iota((256, 16), 0) // 16 == iota((256, 16), 1))
            columns = zero_one((iota((128, 256), 0) // 4 == iota((128, 256), 1) % 4) & (iota((128, 256), 0) < 16))
            for a in range(4):
                rows = jnp.dot(spread, chosen[16 * a : 16 * a + 16], preferred_element_type=jnp.float32)
                rows = jnp.where(iota((256, 128), 0) % 4 == iota((256, 128), 1) % 4, rows, 0.0).astype(jnp.bfloat16)
                full = jnp.dot(rows, columns, preferred_element_type=jnp.float32)
                same = iota((256, 256), 0) // 16 == iota((256, 256), 1) // 16
                weight[q, a] = jnp.where(same, full, 0.0).astype(jnp.bfloat16)

    def units(a):
        for t in range(4 * a, 4 * a + 4):
            for n, (gh, fl) in enumerate(COLUMN + ((0, 0),)):
                arrived(con_all.at[1, gh, t, fl], p_rs.at[n, t])
        for q in (0, 1):

            def quarter(n, carry):
                gc, gh = n // 2, n % 2
                g = ((h + gh) % 2) * 2 + (c + gc) % 2
                lhs = con_all[gc, gh, 4 * a : 4 * a + 4, :, q].reshape(256, 512)
                rhs = w[q, pl.ds(pl.multiple_of(g * 512, 512), 512), :]
                acc[...] += jnp.dot(lhs, rhs, preferred_element_type=jnp.float32)
                return carry

            acc[...] = jnp.zeros_like(acc)
            lax.fori_loop(0, 4, quarter, 0)
            unit[q, a] = acc[...].astype(jnp.bfloat16)

    def terms(a):
        for t in range(4 * a, 4 * a + 4):
            for fl in (0, 1):
                if t or fl:
                    arrived(val_all.at[t * 2 + fl], val_rs.at[t * 2 + fl])
        total = jnp.zeros((256, 256), jnp.float32)
        for q in (0, 1):
            vals = val_all[8 * a : 8 * a + 8, q].reshape(256, 512)
            full = lax.dot_general(unit[q, a], vals, (((1,), (1,)), ((), ())), preferred_element_type=jnp.float32)
            total = total + full * weight[q, a].astype(jnp.float32)
        lanes = iota((256, 128), 1)
        columns = jnp.where(((iota((256, 128), 0) // 4) % 4 == lanes // 4) & (lanes < 16), 1.0, 0.0)
        summed = jnp.dot(total, columns, preferred_element_type=jnp.float32, precision=lax.Precision.HIGHEST)
        summed = jnp.where((iota((256, 128), 0) // 4) % 4 == lanes % 4, summed, 0.0)
        part[4 * a : 4 * a + 4] = jnp.sum(summed.reshape(16, 16, 128), axis=1).reshape(4, 2, 2, 128)

    for step in range(1, 16):
        relay(step)
        if step >= LAG:
            forward(step - LAG)
        if step == 3:
            loads[2].wait()
            weights()
        done = step - LAG - 1
        if done >= 3 and done % 4 == 3:
            units(done // 4)
    for t in range(16 - LAG, 16):
        forward(t)
    units(3)
    for a in range(4):
        terms(a)

    res[0] = part[0, 0]
    for t, (dx, dz) in enumerate(ORDER):
        for fl in (0, 1):
            if t or fl:
                send(part.at[t, fl], res.at[t * 2 + fl], res_ss, res_rs, dev(-dx, -dz, fl))
    arrived(res.at[pl.ds(1, 31)], res_rs)
    fin[ga] = jnp.sum(res[...], axis=0)
    for n, (gh, gc) in enumerate(((0, 1), (1, 0), (1, 1))):
        send(fin.at[ga], fin.at[ga], fin_ss.at[n], fin_rs, dev(0, 0, 0, gh, gc))
    arrived(fin.at[pl.ds(1, 3)], fin_rs)
    total = jnp.sum(fin[...], axis=0)
    out_ref[...] = total[:, :16] / 64.0

    def sent(src, ss):
        pltpu.make_async_copy(src, src, ss).wait()

    sent(d_send.at[pl.ds(1, 15)], con_ss.at[0])
    sent(s_send.at[pl.ds(1, 15)], con_ss.at[1])
    for n in range(3):
        sent(transit, relay_ss.at[n])
    for n in range(4):
        sent(transit, d2d_ss.at[n])
    sent(val_send.at[pl.ds(1, 31)], val_ss)
    sent(qa_all.at[pl.ds(1, 31)], qa_ss)
    sent(res.at[pl.ds(1, 31)], res_ss)
    for n in range(3):
        sent(fin.at[0], fin_ss.at[n])


def body(pair_val, pair_con, screened, amplitude, qmap):
    partner = inverse_rows(qmap)
    qa = jnp.concatenate(
        [qmap.astype(jnp.float32), amplitude.astype(jnp.float32), jnp.zeros((2, 48), jnp.float32)], axis=1
    )
    bf16, f32 = jnp.bfloat16, jnp.float32
    block = (2, 2, 16, 512)
    dma = pltpu.SemaphoreType.DMA
    any_space = pl.BlockSpec(memory_space=pl.ANY)
    vmem = pl.BlockSpec(memory_space=pltpu.VMEM)
    return pl.pallas_call(
        kernel,
        out_shape=jax.ShapeDtypeStruct((2, 16), f32),
        in_specs=[pl.BlockSpec(memory_space=pltpu.SMEM), any_space, any_space, any_space, vmem],
        out_specs=vmem,
        scratch_shapes=[
            pltpu.VMEM((2, 64, 16, 512), bf16),
            pltpu.VMEM((2, 64, 16, 512), bf16),
            pltpu.VMEM((2, 2048, 512), bf16),
            pltpu.VMEM((16, *block), bf16),
            pltpu.VMEM((16, *block), bf16),
            pltpu.VMEM((32, *block), bf16),
            pltpu.VMEM((2, 2, 16, 2, *block), bf16),
            pltpu.VMEM((32, *block), bf16),
            pltpu.VMEM((16, *block), bf16),
            pltpu.VMEM((2, 4, 256, 512), bf16),
            pltpu.VMEM((256, 512), f32),
            pltpu.VMEM((2, 4, 256, 256), bf16),
            pltpu.VMEM((32, 2, 128), f32),
            pltpu.VMEM((16, 2, 2, 128), f32),
            pltpu.VMEM((32, 2, 128), f32),
            pltpu.VMEM((4, 2, 128), f32),
            dma((3,)), dma((16,)), dma((16,)), dma((3, 16)), dma((4, 16)), dma((32,)), dma, dma, dma,
            dma((2,)), dma, dma((3,)), dma((4,)), dma, dma, dma((3,)),
        ],
        compiler_params=pltpu.CompilerParams(collective_id=0, has_side_effects=True),
    )(partner, pair_con, pair_val, screened, qa)


def solution(mesh):
    placed = (
        P("blk", None, None, "ga"),
        P("blk", None, None, "ga"),
        P("blk", None, "ga"),
        P("blk", None),
        P("blk", None),
    )
    return jax.shard_map(
        body, mesh=mesh, in_specs=placed, out_specs=P("blk", None), check_vma=False
    )
```

```python
import jax
import jax.numpy as jnp
from jax import lax
from jax.experimental import pallas as pl
from jax.experimental.pallas import tpu as pltpu
from jax.sharding import PartitionSpec as P

MESH = pl.DeviceIdType.MESH
ORDER = ((2, 2), (1, 1), (3, 3), (1, 3), (3, 1), (2, 1), (1, 2), (2, 3), (3, 2), (2, 0), (0, 2), (0, 3), (1, 0), (3, 0), (0, 1), (0, 0))
HERE = 15
GROUPS = ((0, 4), (4, 4), (8, 4), (12, 3), (15, 1))
QUARTERS = ((0, 0), (0, 1), (1, 0), (1, 1))
COLUMN = ((0, 1), (1, 1), (1, 0))


def iota(shape, dim):
    return lax.broadcasted_iota(jnp.int32, shape, dim)


def zero_one(cond):
    return jnp.where(cond, 1.0, 0.0).astype(jnp.bfloat16)


def hops(offset):
    dx, dz, fl, gh, _ = offset
    return min(dx, 4 - dx) + min(dz, 4 - dz) + (2 if gh and not fl else fl)


def kernel(
    con_hbm, val_hbm, w_hbm, amp_ref, qmap_ref, out_ref,
    con_raw, val_raw, w, s_send, d_send, vs_send, vd_send, con_all, val_all, transit, val_transit,
    acc, weight, rows_ref, partner, qa_all, part, res, fin, last,
    load_sem, s_rs, d_rs, y_rs, p_rs, val_rs, vt_rs, qa_rs, res_rs, fin_rs, last_rs,
    con_ss, val_ss, relay_ss, d2d_ss, qa_ss, res_ss, fin_ss, last_ss,
):
    blk, ga = lax.axis_index("blk"), lax.axis_index("ga")
    lo, x, z = blk // 16, (blk // 4) % 4, blk % 4
    h, c = ga // 2, ga % 2

    def dev(dx, dz, flip_lo=0, flip_h=0, flip_c=0):
        to_lo = (lo + flip_lo) % 2
        to_h = (h + flip_h) % 2
        to_c = (c + flip_c) % 2
        return (to_lo * 16 + ((x + dx + 4) % 4) * 4 + (z + dz + 4) % 4, to_h * 2 + to_c)

    loads = [
        pltpu.make_async_copy(con_hbm, con_raw, load_sem.at[0]),
        pltpu.make_async_copy(val_hbm, val_raw, load_sem.at[1]),
        pltpu.make_async_copy(w_hbm, w, load_sem.at[2]),
    ]
    for load in loads:
        load.start()

    peers = {(dx, dz, fl, 0, 0) for dx, dz in ORDER for fl in (0, 1)}
    peers |= {((4 - dx) % 4, (4 - dz) % 4, fl, gh, gc) for dx, dz in ORDER[12:] for fl in (0, 1) for gh in (0, 1) for gc in (0, 1)}
    peers |= {(dx, dz, fl, gh, gc) for dx, dz in ORDER[12:] for fl in (0, 1) for gh in (0, 1) for gc in (0, 1)}
    peers = sorted(peers - {(0, 0, 0, 0, 0)}, key=lambda p: (-hops(p), p))
    barrier = pltpu.get_barrier_semaphore()
    for offset in peers:
        pl.semaphore_signal(barrier, inc=1, device_id=dev(*offset), device_id_type=MESH)

    def send(src, dst, ss, rs, to):
        pltpu.make_async_remote_copy(src, dst, ss, rs, device_id=to, device_id_type=MESH).start()

    def arrived(dst, rs):
        pltpu.make_async_copy(dst, dst, rs).wait()

    sent = arrived

    qmap = qmap_ref[...]
    for k in (0, 1):
        hit = qmap[k : k + 1, :] == iota((64, 64), 0)
        column = jnp.max(jnp.where(hit, iota((64, 64), 1), 0), axis=1, keepdims=True)
        square = jnp.where(iota((64, 64), 0) == iota((64, 64), 1), column, 0)
        rows_ref[k : k + 1, :] = jnp.max(square, axis=0, keepdims=True)
    to_smem = pltpu.make_async_copy(rows_ref, partner, load_sem.at[3])
    to_smem.start()
    place = zero_one(iota((16, 128), 0) + 64 == iota((16, 128), 1))
    moved = jnp.dot(amp_ref[...], place, preferred_element_type=jnp.float32)
    qa_all[blk] = moved + jnp.concatenate([qmap.astype(jnp.float32), jnp.zeros((2, 64), jnp.float32)], axis=1)
    to_smem.wait()

    loads[0].wait()
    for t, (dx, dz) in enumerate(ORDER):
        for fl, buffer in ((1, d_send), (0, s_send)):
            first = dev(dx, dz, fl)[0] * 2
            for q in (0, 1):
                for k in (0, 1):
                    tile = con_raw[k, partner[k, first + q]]
                    if t != HERE:
                        buffer[t, q, k] = tile
                    elif fl:
                        transit[HERE, q, k] = tile
                    else:
                        con_all[0, 0, HERE, 0, q, k] = tile
    loads[1].wait()
    for t, (dx, dz) in enumerate(ORDER):
        for fl, buffer in ((1, vd_send), (0, vs_send)):
            first = dev(dx, dz, fl)[0] * 2
            for q in (0, 1):
                for k in (0, 1):
                    tile = val_raw[k, partner[k, first + q]]
                    if t == HERE and not fl:
                        val_all[2 * HERE, q, k] = tile
                    else:
                        buffer[t, q, k] = tile
    pl.semaphore_wait(barrier, len(peers))

    def val_along_y(t):
        if t == HERE:
            send(vd_send.at[t], val_all.at[2 * t + 1], val_ss.at[1], val_rs.at[2 * t + 1], dev(0, 0, 1))
        else:
            send(vd_send.at[t], val_transit.at[t], val_ss.at[1], vt_rs.at[t], dev(0, 0, 1))

    def val_onward(t):
        arrived(val_transit.at[t], vt_rs.at[t])
        send(val_transit.at[t], val_all.at[2 * t + 1], val_ss.at[2], val_rs.at[2 * t + 1], dev(*ORDER[t]))

    for t in range(16):
        val_along_y(t)
    for block in range(0, 15, 4):
        for t in range(block, min(block + 4, 15)):
            send(d_send.at[t], transit.at[t], con_ss.at[0], d_rs.at[t], dev(*ORDER[t]))
        for t in range(block, min(block + 4, 15)):
            send(s_send.at[t], con_all.at[0, 0, t, 0], con_ss.at[1], s_rs.at[t], dev(*ORDER[t]))
    for t in range(15):
        send(vs_send.at[t], val_all.at[2 * t], val_ss.at[0], val_rs.at[2 * t], dev(*ORDER[t]))
    for t, (dx, dz) in enumerate(ORDER):
        for fl in (0, 1):
            if t != HERE or fl:
                send(qa_all.at[blk], qa_all.at[blk], qa_ss, qa_rs, dev(dx, dz, fl))

    def relay(t):
        if t != HERE:
            arrived(transit.at[t], d_rs.at[t])
        send(transit.at[t], con_all.at[0, 0, t, 1], relay_ss.at[0], y_rs.at[0, t], dev(0, 0, 1))
        send(transit.at[t], con_all.at[0, 1, t, 1], relay_ss.at[1], y_rs.at[1, t], dev(0, 0, 1, 1))
        here = con_all.at[0, 0, t, 0]
        if t != HERE:
            arrived(here, s_rs.at[t])
        send(here, con_all.at[0, 1, t, 0], relay_ss.at[2], y_rs.at[2, t], dev(0, 0, 0, 1))
        send(here, con_all.at[1, 0, t, 0], d2d_ss.at[3], p_rs.at[3, t], dev(0, 0, 0, 0, 1))

    def forward(t, n):
        gh, fl = COLUMN[n]
        arrived(con_all.at[0, gh, t, fl], y_rs.at[n, t])
        send(con_all.at[0, gh, t, fl], con_all.at[1, gh, t, fl], d2d_ss.at[n], p_rs.at[n, t], dev(0, 0, 0, 0, 1))

    def weights():
        arrived(qa_all.at[pl.ds(1, 31)], qa_rs)
        every = qa_all[...].reshape(64, 128)
        amps = every.astype(jnp.bfloat16)
        pick = zero_one(iota((128, 128), 0) == iota((128, 128), 1) + 64)
        amps = jnp.dot(amps, pick, preferred_element_type=jnp.float32).astype(jnp.bfloat16)
        row = iota((64, 64), 0)
        source = jnp.zeros((64, 64), jnp.int32)
        for t, (dx, dz) in enumerate(ORDER):
            for fl in (0, 1):
                source = jnp.where(row // 2 == t * 2 + fl, dev(-dx, -dz, fl)[0] * 2, source)
        perm = zero_one(source + row % 2 == iota((64, 64), 1))
        for q in (0, 1):
            mine = (blk * 2 + q).astype(jnp.float32)
            hot = zero_one(every[:, :64] == mine)
            chosen = jnp.dot(hot, amps, preferred_element_type=jnp.float32).astype(jnp.bfloat16)
            chosen = jnp.dot(perm, chosen, preferred_element_type=jnp.float32).astype(jnp.bfloat16)
            spread = zero_one(iota((256, 16), 0) // 16 == iota((256, 16), 1))
            columns = zero_one((iota((128, 256), 0) // 4 == iota((128, 256), 1) % 4) & (iota((128, 256), 0) < 16))
            for t0, n in GROUPS:
                rows = jnp.dot(spread[: 64 * n, : 4 * n], chosen[4 * t0 : 4 * (t0 + n)], preferred_element_type=jnp.float32)
                rows = jnp.where(iota((64 * n, 128), 0) % 4 == iota((64 * n, 128), 1) % 4, rows, 0.0).astype(jnp.bfloat16)
                full = jnp.dot(rows, columns, preferred_element_type=jnp.float32)
                same = iota((64 * n, 256), 0) // 16 == iota((64 * n, 256), 1) // 16
                weight[q, 64 * t0 : 64 * (t0 + n)] = jnp.where(same, full, 0.0).astype(jnp.bfloat16)

    def from_partner(t0, n, gh):
        for t in range(t0, t0 + n):
            for m, (of_h, fl) in enumerate(COLUMN + ((0, 0),)):
                if of_h == gh:
                    arrived(con_all.at[1, gh, t, fl], p_rs.at[m, t])

    def quarter(t0, n, gc, gh, first=False):
        g = ((h + gh) % 2) * 2 + (c + gc) % 2

        def one(q, carry):
            lhs = con_all[gc, gh, t0 : t0 + n, :, q].reshape(64 * n, 512)
            rhs = w[q, pl.ds(pl.multiple_of(g * 512, 512), 512), :]
            product = jnp.dot(lhs, rhs, preferred_element_type=jnp.float32)
            if first:
                acc[q, : 64 * n] = product
            else:
                acc[q, : 64 * n] += product
            return carry

        lax.fori_loop(0, 2, one, 0)

    def units(t0, n):
        for gc, gh in QUARTERS:
            if gc:
                from_partner(t0, n, gh)
            quarter(t0, n, gc, gh, first=(gc, gh) == (0, 0))

    def terms(t0, n):
        for t in range(t0, t0 + n):
            for fl in (0, 1):
                if t != HERE or fl:
                    arrived(val_all.at[t * 2 + fl], val_rs.at[t * 2 + fl])
        size = 64 * n
        total = jnp.zeros((size, size), jnp.float32)
        for q in (0, 1):
            vals = val_all[2 * t0 : 2 * (t0 + n), q].reshape(size, 512)
            unit = acc[q, :size].astype(jnp.bfloat16)
            full = lax.dot_general(unit, vals, (((1,), (1,)), ((), ())), preferred_element_type=jnp.float32)
            total = total + full * weight[q, 64 * t0 : 64 * (t0 + n), :size].astype(jnp.float32)
        lanes = iota((size, 128), 1)
        columns = jnp.where(((iota((size, 128), 0) // 4) % 4 == lanes // 4) & (lanes < 16), 1.0, 0.0)
        summed = jnp.dot(total, columns, preferred_element_type=jnp.float32, precision=lax.Precision.HIGHEST)
        summed = jnp.where((iota((size, 128), 0) // 4) % 4 == lanes % 4, summed, 0.0)
        part[2 * t0 : 2 * (t0 + n)] = jnp.sum(summed.reshape(4 * n, 16, 128), axis=1).reshape(2 * n, 2, 128)

    def home(t0, n, ss, rs):
        for t in range(t0, t0 + n):
            dx, dz = ORDER[t]
            for fl in (0, 1):
                for gh in (0, 1):
                    for gc in (0, 1):
                        if (dx, dz, fl, gh, gc) != (0, 0, 0, 0, 0):
                            slot = ((t - 12) * 2 + fl) * 4 + ga
                            send(part.at[t * 2 + fl], last.at[slot], ss, rs, dev(-dx, -dz, fl, gh, gc))

    for t in range(16):
        relay(t)
        if t != HERE:
            val_onward(t)
    weights()
    loads[2].wait()
    for t in range(15):
        for n in range(3):
            forward(t, n)
        if t in (5, 9, 13):
            units(t - 5, 4)
            terms(t - 5, 4)
        if t == 13:
            for u, (dx, dz) in enumerate(ORDER[:12]):
                for fl in (0, 1):
                    send(part.at[u * 2 + fl], res.at[u * 2 + fl], res_ss, res_rs, dev(-dx, -dz, fl))
    units(12, 3)
    terms(12, 3)
    home(12, 3, last_ss.at[0], last_rs.at[0])
    forward(HERE, 1)
    forward(HERE, 2)
    quarter(HERE, 1, 0, 1, True)
    forward(HERE, 0)
    quarter(HERE, 1, 0, 0)
    from_partner(HERE, 1, 1)
    quarter(HERE, 1, 1, 1)
    from_partner(HERE, 1, 0)
    quarter(HERE, 1, 1, 0)
    terms(HERE, 1)
    last[24 + ga] = part[30]
    home(HERE, 1, last_ss.at[1], last_rs.at[1])
    arrived(res, res_rs)
    fin[ga] = jnp.sum(res[...], axis=0)
    for n, (gh, gc) in enumerate(((0, 1), (1, 0), (1, 1))):
        send(fin.at[ga], fin.at[ga], fin_ss.at[n], fin_rs, dev(0, 0, 0, gh, gc))
    arrived(fin.at[pl.ds(1, 3)], fin_rs)
    arrived(last.at[pl.ds(0, 24)], last_rs.at[0])
    arrived(last.at[pl.ds(25, 7)], last_rs.at[1])
    total = jnp.sum(fin[...], axis=0) + jnp.sum(last[...], axis=0)
    out_ref[...] = total[:, :16] / 64.0

    sent(d_send, con_ss.at[0])
    sent(s_send, con_ss.at[1])
    for n in range(3):
        sent(transit, relay_ss.at[n])
    for n in range(4):
        sent(transit, d2d_ss.at[n])
    sent(vs_send, val_ss.at[0])
    sent(vd_send, val_ss.at[1])
    sent(vs_send, val_ss.at[2])
    sent(qa_all.at[pl.ds(1, 31)], qa_ss)
    sent(res, res_ss)
    for n in range(3):
        sent(fin.at[0], fin_ss.at[n])
    sent(last.at[pl.ds(0, 24)], last_ss.at[0])
    sent(last.at[pl.ds(25, 7)], last_ss.at[1])


def body(pair_val, pair_con, screened, amplitude, qmap):
    bf16, f32, i32 = jnp.bfloat16, jnp.float32, jnp.int32
    block = (2, 2, 16, 512)
    dma = pltpu.SemaphoreType.DMA
    any_space = pl.BlockSpec(memory_space=pl.ANY)
    vmem = pl.BlockSpec(memory_space=pltpu.VMEM)
    return pl.pallas_call(
        kernel,
        out_shape=jax.ShapeDtypeStruct((2, 16), f32),
        in_specs=[any_space, any_space, any_space, vmem, vmem],
        out_specs=vmem,
        scratch_shapes=[
            pltpu.VMEM((2, 64, 16, 512), bf16),
            pltpu.VMEM((2, 64, 16, 512), bf16),
            pltpu.VMEM((2, 2048, 512), bf16),
            pltpu.VMEM((15, *block), bf16),
            pltpu.VMEM((15, *block), bf16),
            pltpu.VMEM((15, *block), bf16),
            pltpu.VMEM((16, *block), bf16),
            pltpu.VMEM((2, 2, 16, 2, *block), bf16),
            pltpu.VMEM((32, *block), bf16),
            pltpu.VMEM((16, *block), bf16),
            pltpu.VMEM((15, *block), bf16),
            pltpu.VMEM((2, 256, 512), f32),
            pltpu.VMEM((2, 1024, 256), bf16),
            pltpu.VMEM((2, 64), i32),
            pltpu.SMEM((2, 64), i32),
            pltpu.VMEM((32, 2, 128), f32),
            pltpu.VMEM((32, 2, 128), f32),
            pltpu.VMEM((24, 2, 128), f32),
            pltpu.VMEM((4, 2, 128), f32),
            pltpu.VMEM((32, 2, 128), f32),
            dma((4,)), dma((16,)), dma((16,)), dma((3, 16)), dma((4, 16)), dma((32,)), dma((16,)), dma, dma, dma, dma((2,)),
            dma((2,)), dma((3,)), dma((3,)), dma((4,)), dma, dma, dma((3,)), dma((2,)),
        ],
        compiler_params=pltpu.CompilerParams(collective_id=0, has_side_effects=True),
    )(pair_con, pair_val, screened, amplitude, qmap)


def solution(mesh):
    placed = (
        P("blk", None, None, "ga"),
        P("blk", None, None, "ga"),
        P("blk", None, "ga"),
        P("blk", None),
        P("blk", None),
    )
    return jax.shard_map(
        body, mesh=mesh, in_specs=placed, out_specs=P("blk", None), check_vma=False
    )
```

```python
import jax
import jax.numpy as jnp
from jax import lax
from jax.experimental import pallas as pl
from jax.experimental.pallas import tpu as pltpu
from jax.sharding import PartitionSpec as P

MESH = pl.DeviceIdType.MESH
ORDER = ((2, 2), (1, 1), (3, 3), (1, 3), (3, 1), (2, 1), (1, 2), (2, 3), (3, 2), (2, 0), (0, 2), (0, 3), (1, 0), (3, 0), (0, 1), (0, 0))
HERE = 15
GROUPS = ((0, 4), (4, 4), (8, 4), (12, 3), (15, 1))
QUARTERS = ((0, 0), (0, 1), (1, 0), (1, 1))
COLUMN = ((0, 1), (1, 1), (1, 0))


def iota(shape, dim):
    return lax.broadcasted_iota(jnp.int32, shape, dim)


def zero_one(cond):
    return jnp.where(cond, 1.0, 0.0).astype(jnp.bfloat16)


def kernel(
    con_hbm, val_hbm, w_hbm, amp_ref, qmap_ref, out_ref,
    con_raw, val_raw, w, s_send, d_send, vs_send, vd_send, con_all, val_all, transit, val_transit,
    acc, weight, rows_ref, partner, qa_all, part, res, fin, last,
    ready, load_sem, s_rs, d_rs, y_rs, p_rs, val_rs, vt_rs, qa_rs, res_rs, fin_rs, last_rs,
    con_ss, val_ss, relay_ss, d2d_ss, qa_ss, res_ss, fin_ss, last_ss,
):
    blk, ga = lax.axis_index("blk"), lax.axis_index("ga")
    lo, x, z = blk // 16, (blk // 4) % 4, blk % 4
    h, c = ga // 2, ga % 2

    def dev(dx, dz, flip_lo=0, flip_h=0, flip_c=0):
        to_lo = (lo + flip_lo) % 2
        to_h = (h + flip_h) % 2
        to_c = (c + flip_c) % 2
        return (to_lo * 16 + ((x + dx + 4) % 4) * 4 + (z + dz + 4) % 4, to_h * 2 + to_c)

    loads = [
        pltpu.make_async_copy(con_hbm, con_raw, load_sem.at[0]),
        pltpu.make_async_copy(val_hbm, val_raw, load_sem.at[1]),
        pltpu.make_async_copy(w_hbm, w, load_sem.at[2]),
    ]
    along_x = [(d, 0, 0, 0, 0) for d in (2, 1, 3)]
    along_z = [(0, d, 0, 0, 0) for d in (2, 1, 3)]
    along_y = [(0, 0, 0, 1, 0), (0, 0, 1, 0, 0), (0, 0, 1, 1, 0)]
    other_core = [(0, 0, 0, 0, 1)]
    lines = along_x + along_z + along_y + other_core
    barrier = pltpu.get_barrier_semaphore()
    for offset in lines:
        pl.semaphore_signal(barrier, inc=1, device_id=dev(*offset), device_id_type=MESH)
    loads[1].start()
    loads[0].start()

    def tell(stage, group):
        for offset in group:
            pl.semaphore_signal(ready.at[stage], inc=1, device_id=dev(*offset), device_id_type=MESH)

    def send(src, dst, ss, rs, to):
        pltpu.make_async_remote_copy(src, dst, ss, rs, device_id=to, device_id_type=MESH).start()

    def arrived(dst, rs):
        pltpu.make_async_copy(dst, dst, rs).wait()

    sent = arrived

    qmap = qmap_ref[...]
    for k in (0, 1):
        hit = qmap[k : k + 1, :] == iota((64, 64), 0)
        column = jnp.max(jnp.where(hit, iota((64, 64), 1), 0), axis=1, keepdims=True)
        square = jnp.where(iota((64, 64), 0) == iota((64, 64), 1), column, 0)
        rows_ref[k : k + 1, :] = jnp.max(square, axis=0, keepdims=True)
    to_smem = pltpu.make_async_copy(rows_ref, partner, load_sem.at[3])
    to_smem.start()
    place = zero_one(iota((16, 128), 0) + 64 == iota((16, 128), 1))
    moved = jnp.dot(amp_ref[...], place, preferred_element_type=jnp.float32)
    qa_all[blk] = moved + jnp.concatenate([qmap.astype(jnp.float32), jnp.zeros((2, 64), jnp.float32)], axis=1)
    to_smem.wait()

    def ordered(raw, k, q, dx, dz, fl):
        return raw[k, partner[k, dev(dx, dz, fl)[0] * 2 + q]]

    loads[1].wait()
    for fl, buffer in ((1, vd_send), (0, vs_send)):
        for t, (dx, dz) in enumerate(ORDER):
            for q in (0, 1):
                for k in (0, 1):
                    tile = ordered(val_raw, k, q, dx, dz, fl)
                    if t == HERE and not fl:
                        val_all[2 * HERE, q, k] = tile
                    else:
                        buffer[t, q, k] = tile
    pl.semaphore_wait(barrier, len(lines))
    tell(0, along_x)

    def val_along_y(t):
        if t == HERE:
            send(vd_send.at[t], val_all.at[2 * t + 1], val_ss.at[1], val_rs.at[2 * t + 1], dev(0, 0, 1))
        else:
            send(vd_send.at[t], val_transit.at[t], val_ss.at[1], vt_rs.at[t], dev(0, 0, 1))

    def val_onward(t):
        arrived(val_transit.at[t], vt_rs.at[t])
        send(val_transit.at[t], val_all.at[2 * t + 1], val_ss.at[2], val_rs.at[2 * t + 1], dev(*ORDER[t]))

    for t in range(15):
        val_along_y(t)
    loads[0].wait()
    for t, (dx, dz) in enumerate(ORDER):
        for fl, buffer in ((1, d_send), (0, s_send)):
            for q in (0, 1):
                for k in (0, 1):
                    tile = ordered(con_raw, k, q, dx, dz, fl)
                    if t != HERE:
                        buffer[t, q, k] = tile
                    elif fl:
                        transit[HERE, q, k] = tile
                    else:
                        con_all[0, 0, HERE, 0, q, k] = tile
    loads[2].start()
    pl.semaphore_wait(ready.at[0], 3)
    tell(1, along_z)
    for block in range(0, 15, 4):
        for t in range(block, min(block + 4, 15)):
            send(d_send.at[t], transit.at[t], con_ss.at[0], d_rs.at[t], dev(*ORDER[t]))
        for t in range(block, min(block + 4, 15)):
            send(s_send.at[t], con_all.at[0, 0, t, 0], con_ss.at[1], s_rs.at[t], dev(*ORDER[t]))
        if block == 4:
            pl.semaphore_wait(ready.at[1], 3)
            tell(2, other_core)
            for t, (dx, dz) in enumerate(ORDER):
                for fl in (0, 1):
                    if t != HERE or fl:
                        send(qa_all.at[blk], qa_all.at[blk], qa_ss, qa_rs, dev(dx, dz, fl))
    for t in range(15):
        send(vs_send.at[t], val_all.at[2 * t], val_ss.at[0], val_rs.at[2 * t], dev(*ORDER[t]))
    pl.semaphore_wait(ready.at[2], 1)

    def relay_d(t):
        if t != HERE:
            arrived(transit.at[t], d_rs.at[t])
        send(transit.at[t], con_all.at[0, 0, t, 1], relay_ss.at[0], y_rs.at[0, t], dev(0, 0, 1))
        send(transit.at[t], con_all.at[0, 1, t, 1], relay_ss.at[1], y_rs.at[1, t], dev(0, 0, 1, 1))

    def relay_s(t):
        here = con_all.at[0, 0, t, 0]
        if t != HERE:
            arrived(here, s_rs.at[t])
        send(here, con_all.at[0, 1, t, 0], relay_ss.at[2], y_rs.at[2, t], dev(0, 0, 0, 1))
        send(here, con_all.at[1, 0, t, 0], d2d_ss.at[3], p_rs.at[3, t], dev(0, 0, 0, 0, 1))

    def forward(t, n):
        gh, fl = COLUMN[n]
        arrived(con_all.at[0, gh, t, fl], y_rs.at[n, t])
        send(con_all.at[0, gh, t, fl], con_all.at[1, gh, t, fl], d2d_ss.at[n], p_rs.at[n, t], dev(0, 0, 0, 0, 1))

    def weights():
        arrived(qa_all.at[pl.ds(1, 31)], qa_rs)
        every = qa_all[...].reshape(64, 128)
        amps = every.astype(jnp.bfloat16)
        pick = zero_one(iota((128, 128), 0) == iota((128, 128), 1) + 64)
        amps = jnp.dot(amps, pick, preferred_element_type=jnp.float32).astype(jnp.bfloat16)
        row = iota((64, 64), 0)
        source = jnp.zeros((64, 64), jnp.int32)
        for t, (dx, dz) in enumerate(ORDER):
            for fl in (0, 1):
                source = jnp.where(row // 2 == t * 2 + fl, dev(-dx, -dz, fl)[0] * 2, source)
        perm = zero_one(source + row % 2 == iota((64, 64), 1))
        for q in (0, 1):
            mine = (blk * 2 + q).astype(jnp.float32)
            hot = zero_one(every[:, :64] == mine)
            chosen = jnp.dot(hot, amps, preferred_element_type=jnp.float32).astype(jnp.bfloat16)
            chosen = jnp.dot(perm, chosen, preferred_element_type=jnp.float32).astype(jnp.bfloat16)
            spread = zero_one(iota((256, 16), 0) // 16 == iota((256, 16), 1))
            columns = zero_one((iota((128, 256), 0) // 4 == iota((128, 256), 1) % 4) & (iota((128, 256), 0) < 16))
            for t0, n in GROUPS:
                rows = jnp.dot(spread[: 64 * n, : 4 * n], chosen[4 * t0 : 4 * (t0 + n)], preferred_element_type=jnp.float32)
                rows = jnp.where(iota((64 * n, 128), 0) % 4 == iota((64 * n, 128), 1) % 4, rows, 0.0).astype(jnp.bfloat16)
                full = jnp.dot(rows, columns, preferred_element_type=jnp.float32)
                same = iota((64 * n, 256), 0) // 16 == iota((64 * n, 256), 1) // 16
                weight[q, 64 * t0 : 64 * (t0 + n)] = jnp.where(same, full, 0.0).astype(jnp.bfloat16)

    def from_partner(t0, n, gh):
        for t in range(t0, t0 + n):
            for m, (of_h, fl) in enumerate(COLUMN + ((0, 0),)):
                if of_h == gh:
                    arrived(con_all.at[1, gh, t, fl], p_rs.at[m, t])

    def quarter(t0, n, gc, gh, first=False):
        g = ((h + gh) % 2) * 2 + (c + gc) % 2

        def one(q, carry):
            lhs = con_all[gc, gh, t0 : t0 + n, :, q].reshape(64 * n, 512)
            rhs = w[q, pl.ds(pl.multiple_of(g * 512, 512), 512), :]
            product = jnp.dot(lhs, rhs, preferred_element_type=jnp.float32)
            if first:
                acc[q, : 64 * n] = product
            else:
                acc[q, : 64 * n] += product
            return carry

        lax.fori_loop(0, 2, one, 0)

    def units(t0, n):
        for gc, gh in QUARTERS:
            if gc:
                from_partner(t0, n, gh)
            quarter(t0, n, gc, gh, first=(gc, gh) == (0, 0))

    def terms(t0, n):
        for t in range(t0, t0 + n):
            for fl in (0, 1):
                if t != HERE or fl:
                    arrived(val_all.at[t * 2 + fl], val_rs.at[t * 2 + fl])
        size = 64 * n
        total = jnp.zeros((size, size), jnp.float32)
        for q in (0, 1):
            vals = val_all[2 * t0 : 2 * (t0 + n), q].reshape(size, 512)
            unit = acc[q, :size].astype(jnp.bfloat16)
            full = lax.dot_general(unit, vals, (((1,), (1,)), ((), ())), preferred_element_type=jnp.float32)
            total = total + full * weight[q, 64 * t0 : 64 * (t0 + n), :size].astype(jnp.float32)
        lanes = iota((size, 128), 1)
        columns = jnp.where(((iota((size, 128), 0) // 4) % 4 == lanes // 4) & (lanes < 16), 1.0, 0.0)
        summed = jnp.dot(total, columns, preferred_element_type=jnp.float32, precision=lax.Precision.HIGHEST)
        summed = jnp.where((iota((size, 128), 0) // 4) % 4 == lanes % 4, summed, 0.0)
        part[2 * t0 : 2 * (t0 + n)] = jnp.sum(summed.reshape(4 * n, 16, 128), axis=1).reshape(2 * n, 2, 128)

    def home(t0, n, ss, rs):
        for t in range(t0, t0 + n):
            dx, dz = ORDER[t]
            for fl in (0, 1):
                for gh in (0, 1):
                    for gc in (0, 1):
                        if (dx, dz, fl, gh, gc) != (0, 0, 0, 0, 0):
                            slot = ((t - 12) * 2 + fl) * 4 + ga
                            send(part.at[t * 2 + fl], last.at[slot], ss, rs, dev(-dx, -dz, fl, gh, gc))

    for t in range(15):
        relay_d(t)
        relay_s(t)
        val_onward(t)
    relay_s(HERE)
    relay_d(HERE)
    val_along_y(HERE)
    weights()
    loads[2].wait()
    for t in range(15):
        for n in range(3):
            forward(t, n)
        if t in (4, 8, 12):
            units(t - 4, 4)
            terms(t - 4, 4)
        if t == 12:
            for u, (dx, dz) in enumerate(ORDER[:12]):
                for fl in (0, 1):
                    send(part.at[u * 2 + fl], res.at[u * 2 + fl], res_ss, res_rs, dev(-dx, -dz, fl))
    quarter(12, 3, 0, 0, True)
    quarter(12, 3, 0, 1)
    forward(HERE, 1)
    forward(HERE, 2)
    from_partner(12, 3, 0)
    quarter(12, 3, 1, 0)
    from_partner(12, 3, 1)
    quarter(12, 3, 1, 1)
    terms(12, 3)
    home(12, 3, last_ss.at[0], last_rs.at[0])
    forward(HERE, 0)
    quarter(HERE, 1, 0, 1, True)
    quarter(HERE, 1, 0, 0)
    from_partner(HERE, 1, 1)
    quarter(HERE, 1, 1, 1)
    arrived(res, res_rs)
    fin[ga] = jnp.sum(res[...], axis=0)
    for n, (gh, gc) in enumerate(((0, 1), (1, 0), (1, 1))):
        send(fin.at[ga], fin.at[ga], fin_ss.at[n], fin_rs, dev(0, 0, 0, gh, gc))
    from_partner(HERE, 1, 0)
    quarter(HERE, 1, 1, 0)
    terms(HERE, 1)
    last[24 + ga] = part[30]
    home(HERE, 1, last_ss.at[1], last_rs.at[1])
    arrived(fin.at[pl.ds(1, 3)], fin_rs)
    arrived(last.at[pl.ds(0, 24)], last_rs.at[0])
    arrived(last.at[pl.ds(25, 7)], last_rs.at[1])
    total = jnp.sum(fin[...], axis=0) + jnp.sum(last[...], axis=0)
    out_ref[...] = total[:, :16] / 64.0

    sent(d_send, con_ss.at[0])
    sent(s_send, con_ss.at[1])
    for n in range(3):
        sent(transit, relay_ss.at[n])
    for n in range(4):
        sent(transit, d2d_ss.at[n])
    sent(vs_send, val_ss.at[0])
    sent(vd_send, val_ss.at[1])
    sent(vs_send, val_ss.at[2])
    sent(qa_all.at[pl.ds(1, 31)], qa_ss)
    sent(res, res_ss)
    for n in range(3):
        sent(fin.at[0], fin_ss.at[n])
    sent(last.at[pl.ds(0, 24)], last_ss.at[0])
    sent(last.at[pl.ds(25, 7)], last_ss.at[1])


def body(pair_val, pair_con, screened, amplitude, qmap):
    bf16, f32, i32 = jnp.bfloat16, jnp.float32, jnp.int32
    block = (2, 2, 16, 512)
    dma = pltpu.SemaphoreType.DMA
    any_space = pl.BlockSpec(memory_space=pl.ANY)
    vmem = pl.BlockSpec(memory_space=pltpu.VMEM)
    return pl.pallas_call(
        kernel,
        out_shape=jax.ShapeDtypeStruct((2, 16), f32),
        in_specs=[any_space, any_space, any_space, vmem, vmem],
        out_specs=vmem,
        scratch_shapes=[
            pltpu.VMEM((2, 64, 16, 512), bf16),
            pltpu.VMEM((2, 64, 16, 512), bf16),
            pltpu.VMEM((2, 2048, 512), bf16),
            pltpu.VMEM((15, *block), bf16),
            pltpu.VMEM((15, *block), bf16),
            pltpu.VMEM((15, *block), bf16),
            pltpu.VMEM((16, *block), bf16),
            pltpu.VMEM((2, 2, 16, 2, *block), bf16),
            pltpu.VMEM((32, *block), bf16),
            pltpu.VMEM((16, *block), bf16),
            pltpu.VMEM((15, *block), bf16),
            pltpu.VMEM((2, 256, 512), f32),
            pltpu.VMEM((2, 1024, 256), bf16),
            pltpu.VMEM((2, 64), i32),
            pltpu.SMEM((2, 64), i32),
            pltpu.VMEM((32, 2, 128), f32),
            pltpu.VMEM((32, 2, 128), f32),
            pltpu.VMEM((24, 2, 128), f32),
            pltpu.VMEM((4, 2, 128), f32),
            pltpu.VMEM((32, 2, 128), f32),
            pltpu.SemaphoreType.REGULAR((3,)), dma((4,)), dma((16,)), dma((16,)), dma((3, 16)), dma((4, 16)), dma((32,)), dma((16,)), dma, dma, dma, dma((2,)),
            dma((2,)), dma((3,)), dma((3,)), dma((4,)), dma, dma, dma((3,)), dma((2,)),
        ],
        compiler_params=pltpu.CompilerParams(collective_id=0, has_side_effects=True),
    )(pair_con, pair_val, screened, amplitude, qmap)


def solution(mesh):
    placed = (
        P("blk", None, None, "ga"),
        P("blk", None, None, "ga"),
        P("blk", None, "ga"),
        P("blk", None),
        P("blk", None),
    )
    return jax.shard_map(
        body, mesh=mesh, in_specs=placed, out_specs=P("blk", None), check_vma=False
    )
```

```python
import jax
import jax.numpy as jnp
from jax import lax
from jax.experimental import pallas as pl
from jax.experimental.pallas import tpu as pltpu
from jax.sharding import PartitionSpec as P

MESH = pl.DeviceIdType.MESH
ORDER = ((2, 2), (1, 1), (3, 3), (1, 3), (3, 1), (2, 1), (1, 2), (2, 3), (3, 2), (2, 0), (0, 2), (0, 3), (1, 0), (3, 0), (0, 1), (0, 0))
HERE = 15
GROUPS = ((0, 4), (4, 4), (8, 4), (12, 2), (14, 1), (15, 1))
COLUMN = ((0, 1), (1, 1), (1, 0))


def iota(shape, dim):
    return lax.broadcasted_iota(jnp.int32, shape, dim)


def zero_one(cond):
    return jnp.where(cond, 1.0, 0.0).astype(jnp.bfloat16)


def kernel(
    con_hbm, val_hbm, w_hbm, amp_hbm, qmap_hbm, out_ref,
    amp_ref, qmap_ref, con_raw, val_raw, w, s_send, d_send, vs_send, vd_send, con_all, val_all, transit, val_transit,
    acc, weight, rows_ref, partner, qa_all, part, every,
    ready, load_sem, s_rs, d_rs, y_rs, p_rs, val_rs, vt_rs, qa_rs, home_rs,
    con_ss, val_ss, relay_ss, d2d_ss, qa_ss, home_ss,
):
    blk, ga = lax.axis_index("blk"), lax.axis_index("ga")
    lo, x, z = blk // 16, (blk // 4) % 4, blk % 4
    h, c = ga // 2, ga % 2

    def dev(dx, dz, flip_lo=0, flip_h=0, flip_c=0):
        to_lo = (lo + flip_lo) % 2
        to_h = (h + flip_h) % 2
        to_c = (c + flip_c) % 2
        return (to_lo * 16 + ((x + dx + 4) % 4) * 4 + (z + dz + 4) % 4, to_h * 2 + to_c)

    loads = [
        pltpu.make_async_copy(con_hbm, con_raw, load_sem.at[0]),
        pltpu.make_async_copy(val_hbm, val_raw, load_sem.at[1]),
        pltpu.make_async_copy(w_hbm, w, load_sem.at[2]),
        pltpu.make_async_copy(qmap_hbm, qmap_ref, load_sem.at[3]),
        pltpu.make_async_copy(amp_hbm, amp_ref, load_sem.at[4]),
    ]
    along_x = [(d, 0, 0, 0, 0) for d in (2, 1, 3)]
    along_z = [(0, d, 0, 0, 0) for d in (2, 1, 3)]
    along_y = [(0, 0, 0, 1, 0), (0, 0, 1, 0, 0), (0, 0, 1, 1, 0)]
    other_core = [(0, 0, 0, 0, 1)]
    lines = along_y + along_x + along_z + other_core
    barrier = pltpu.get_barrier_semaphore()
    for offset in lines:
        pl.semaphore_signal(barrier, inc=1, device_id=dev(*offset), device_id_type=MESH)
    for n in (3, 4, 1, 0):
        loads[n].start()

    def tell(stage, group):
        for offset in group:
            pl.semaphore_signal(ready.at[stage], inc=1, device_id=dev(*offset), device_id_type=MESH)

    def send(src, dst, ss, rs, to):
        pltpu.make_async_remote_copy(src, dst, ss, rs, device_id=to, device_id_type=MESH).start()

    def arrived(dst, rs):
        pltpu.make_async_copy(dst, dst, rs).wait()

    sent = arrived

    loads[3].wait()
    qmap = qmap_ref[...]
    for k in (0, 1):
        hit = qmap[k : k + 1, :] == iota((64, 64), 0)
        column = jnp.max(jnp.where(hit, iota((64, 64), 1), 0), axis=1, keepdims=True)
        square = jnp.where(iota((64, 64), 0) == iota((64, 64), 1), column, 0)
        rows_ref[k : k + 1, :] = jnp.max(square, axis=0, keepdims=True)
    to_smem = pltpu.make_async_copy(rows_ref, partner, load_sem.at[5])
    to_smem.start()
    loads[4].wait()
    place = zero_one(iota((16, 128), 0) + 64 == iota((16, 128), 1))
    moved = jnp.dot(amp_ref[...], place, preferred_element_type=jnp.float32)
    qa_all[blk] = moved + jnp.concatenate([qmap.astype(jnp.float32), jnp.zeros((2, 64), jnp.float32)], axis=1)
    to_smem.wait()

    def ordered(raw, k, q, dx, dz, fl):
        return raw[k, partner[k, dev(dx, dz, fl)[0] * 2 + q]]

    loads[1].wait()
    for fl, buffer in ((1, vd_send), (0, vs_send)):
        for t, (dx, dz) in enumerate(ORDER):
            for q in (0, 1):
                for k in (0, 1):
                    tile = ordered(val_raw, k, q, dx, dz, fl)
                    if t == HERE and not fl:
                        val_all[2 * HERE, q, k] = tile
                    else:
                        buffer[t, q, k] = tile
    pl.semaphore_wait(barrier, len(lines))
    tell(0, along_x)

    def val_along_y(t):
        if t == HERE:
            send(vd_send.at[t], val_all.at[2 * t + 1], val_ss.at[1], val_rs.at[2 * t + 1], dev(0, 0, 1))
        else:
            send(vd_send.at[t], val_transit.at[t], val_ss.at[1], vt_rs.at[t], dev(0, 0, 1))

    def val_onward(t):
        arrived(val_transit.at[t], vt_rs.at[t])
        send(val_transit.at[t], val_all.at[2 * t + 1], val_ss.at[2], val_rs.at[2 * t + 1], dev(*ORDER[t]))

    for t in range(15):
        val_along_y(t)
    loads[0].wait()
    for t, (dx, dz) in enumerate(ORDER):
        for fl, buffer in ((1, d_send), (0, s_send)):
            for q in (0, 1):
                for k in (0, 1):
                    tile = ordered(con_raw, k, q, dx, dz, fl)
                    if t != HERE:
                        buffer[t, q, k] = tile
                    elif fl:
                        transit[HERE, q, k] = tile
                    else:
                        con_all[0, 0, HERE, 0, q, k] = tile
    loads[2].start()
    pl.semaphore_wait(ready.at[0], 3)
    tell(1, along_z)
    for block in range(0, 15, 4):
        for t in range(block, min(block + 4, 15)):
            send(d_send.at[t], transit.at[t], con_ss.at[0], d_rs.at[t], dev(*ORDER[t]))
        for t in range(block, min(block + 4, 15)):
            send(s_send.at[t], con_all.at[0, 0, t, 0], con_ss.at[1], s_rs.at[t], dev(*ORDER[t]))
        if block == 4:
            pl.semaphore_wait(ready.at[1], 3)
            tell(2, other_core)
            for t, (dx, dz) in enumerate(ORDER):
                for fl in (0, 1):
                    if t != HERE or fl:
                        send(qa_all.at[blk], qa_all.at[blk], qa_ss, qa_rs, dev(dx, dz, fl))
    for t in range(15):
        send(vs_send.at[t], val_all.at[2 * t], val_ss.at[0], val_rs.at[2 * t], dev(*ORDER[t]))
    pl.semaphore_wait(ready.at[2], 1)

    def relay_d(t):
        if t != HERE:
            arrived(transit.at[t], d_rs.at[t])
        send(transit.at[t], con_all.at[0, 0, t, 1], relay_ss.at[0], y_rs.at[0, t], dev(0, 0, 1))
        send(transit.at[t], con_all.at[0, 1, t, 1], relay_ss.at[1], y_rs.at[1, t], dev(0, 0, 1, 1))

    def relay_s(t):
        here = con_all.at[0, 0, t, 0]
        if t != HERE:
            arrived(here, s_rs.at[t])
        send(here, con_all.at[0, 1, t, 0], relay_ss.at[2], y_rs.at[2, t], dev(0, 0, 0, 1))
        send(here, con_all.at[1, 0, t, 0], d2d_ss.at[3], p_rs.at[3, t], dev(0, 0, 0, 0, 1))

    def forward(t, n):
        gh, fl = COLUMN[n]
        arrived(con_all.at[0, gh, t, fl], y_rs.at[n, t])
        send(con_all.at[0, gh, t, fl], con_all.at[1, gh, t, fl], d2d_ss.at[n], p_rs.at[n, t], dev(0, 0, 0, 0, 1))

    def weights():
        arrived(qa_all.at[pl.ds(1, 31)], qa_rs)
        table = qa_all[...].reshape(64, 128)
        amps = table.astype(jnp.bfloat16)
        pick = zero_one(iota((128, 128), 0) == iota((128, 128), 1) + 64)
        amps = jnp.dot(amps, pick, preferred_element_type=jnp.float32).astype(jnp.bfloat16)
        row = iota((64, 64), 0)
        source = jnp.zeros((64, 64), jnp.int32)
        for t, (dx, dz) in enumerate(ORDER):
            for fl in (0, 1):
                source = jnp.where(row // 2 == t * 2 + fl, dev(-dx, -dz, fl)[0] * 2, source)
        perm = zero_one(source + row % 2 == iota((64, 64), 1))
        for q in (0, 1):
            mine = (blk * 2 + q).astype(jnp.float32)
            hot = zero_one(table[:, :64] == mine)
            chosen = jnp.dot(hot, amps, preferred_element_type=jnp.float32).astype(jnp.bfloat16)
            chosen = jnp.dot(perm, chosen, preferred_element_type=jnp.float32).astype(jnp.bfloat16)
            spread = zero_one(iota((256, 16), 0) // 16 == iota((256, 16), 1))
            columns = zero_one((iota((128, 256), 0) // 4 == iota((128, 256), 1) % 4) & (iota((128, 256), 0) < 16))
            for t0, n in GROUPS:
                rows = jnp.dot(spread[: 64 * n, : 4 * n], chosen[4 * t0 : 4 * (t0 + n)], preferred_element_type=jnp.float32)
                rows = jnp.where(iota((64 * n, 128), 0) % 4 == iota((64 * n, 128), 1) % 4, rows, 0.0).astype(jnp.bfloat16)
                full = jnp.dot(rows, columns, preferred_element_type=jnp.float32)
                same = iota((64 * n, 256), 0) // 16 == iota((64 * n, 256), 1) // 16
                weight[q, 64 * t0 : 64 * (t0 + n)] = jnp.where(same, full, 0.0).astype(jnp.bfloat16)

    def from_partner(t0, n, gh):
        for t in range(t0, t0 + n):
            for m, (of_h, fl) in enumerate(COLUMN + ((0, 0),)):
                if of_h == gh:
                    arrived(con_all.at[1, gh, t, fl], p_rs.at[m, t])

    def quarter(t0, n, gc, gh, first=False):
        g = ((h + gh) % 2) * 2 + (c + gc) % 2

        def one(q, carry):
            lhs = con_all[gc, gh, t0 : t0 + n, :, q].reshape(64 * n, 512)
            rhs = w[q, pl.ds(pl.multiple_of(g * 512, 512), 512), :]
            product = jnp.dot(lhs, rhs, preferred_element_type=jnp.float32)
            if first:
                acc[q, : 64 * n] = product
            else:
                acc[q, : 64 * n] += product
            return carry

        lax.fori_loop(0, 2, one, 0)

    def own(t0, n):
        quarter(t0, n, 0, 0, True)
        quarter(t0, n, 0, 1)

    def others(t0, n):
        for gh in (0, 1):
            from_partner(t0, n, gh)
            quarter(t0, n, 1, gh)

    def terms(t0, n):
        for t in range(t0, t0 + n):
            for fl in (0, 1):
                if t != HERE or fl:
                    arrived(val_all.at[t * 2 + fl], val_rs.at[t * 2 + fl])
        size = 64 * n
        total = jnp.zeros((size, size), jnp.float32)
        for q in (0, 1):
            vals = val_all[2 * t0 : 2 * (t0 + n), q].reshape(size, 512)
            unit = acc[q, :size].astype(jnp.bfloat16)
            full = lax.dot_general(unit, vals, (((1,), (1,)), ((), ())), preferred_element_type=jnp.float32)
            total = total + full * weight[q, 64 * t0 : 64 * (t0 + n), :size].astype(jnp.float32)
        lanes = iota((size, 128), 1)
        columns = zero_one(((iota((size, 128), 0) // 4) % 4 == lanes // 4) & (lanes < 16))
        high = total.astype(jnp.bfloat16)
        low = (total - high.astype(jnp.float32)).astype(jnp.bfloat16)
        summed = jnp.dot(high, columns, preferred_element_type=jnp.float32)
        summed = summed + jnp.dot(low, columns, preferred_element_type=jnp.float32)
        summed = jnp.where((iota((size, 128), 0) // 4) % 4 == lanes % 4, summed, 0.0)
        part[2 * t0 : 2 * (t0 + n)] = jnp.sum(summed.reshape(4 * n, 16, 128), axis=1).reshape(2 * n, 2, 128)

    def home(t0, n):
        batch = GROUPS.index((t0, n))
        for t in range(t0, t0 + n):
            dx, dz = ORDER[t]
            for fl in (0, 1):
                for gh in (0, 1):
                    for gc in (0, 1):
                        if (dx, dz, fl, gh, gc) != (0, 0, 0, 0, 0):
                            slot = (t * 2 + fl) * 4 + ga
                            send(part.at[t * 2 + fl], every.at[slot], home_ss.at[batch], home_rs.at[batch], dev(-dx, -dz, fl, gh, gc))

    for t in range(15):
        relay_d(t)
        relay_s(t)
        val_onward(t)
    relay_s(HERE)
    relay_d(HERE)
    val_along_y(HERE)
    weights()
    loads[2].wait()
    for t in range(14):
        for n in range(3):
            forward(t, n)
        if t in (3, 7, 11):
            own(t - 3, 4)
        if t in (4, 8, 12):
            others(t - 4, 4)
            terms(t - 4, 4)
            home(t - 4, 4)
    own(12, 2)
    others(12, 2)
    terms(12, 2)
    home(12, 2)
    for n in range(3):
        forward(14, n)
    own(14, 1)
    others(14, 1)
    terms(14, 1)
    home(14, 1)
    forward(HERE, 1)
    forward(HERE, 2)
    quarter(HERE, 1, 0, 1, True)
    forward(HERE, 0)
    quarter(HERE, 1, 0, 0)
    from_partner(HERE, 1, 1)
    quarter(HERE, 1, 1, 1)
    from_partner(HERE, 1, 0)
    quarter(HERE, 1, 1, 0)
    terms(HERE, 1)
    every[120 + ga] = part[30]
    home(HERE, 1)
    for batch, (t0, n) in enumerate(GROUPS):
        first = 8 * t0 + (t0 == HERE)
        arrived(every.at[pl.ds(first, 8 * (t0 + n) - first)], home_rs.at[batch])
    out_ref[...] = jnp.sum(every[...], axis=0)[:, :16] / 64.0

    sent(d_send, con_ss.at[0])
    sent(s_send, con_ss.at[1])
    for n in range(3):
        sent(transit, relay_ss.at[n])
    for n in range(4):
        sent(transit, d2d_ss.at[n])
    sent(vs_send, val_ss.at[0])
    sent(vd_send, val_ss.at[1])
    sent(vs_send, val_ss.at[2])
    sent(qa_all.at[pl.ds(1, 31)], qa_ss)
    for batch, (t0, n) in enumerate(GROUPS):
        first = 8 * t0 + (t0 == HERE)
        sent(every.at[pl.ds(first, 8 * (t0 + n) - first)], home_ss.at[batch])


def body(pair_val, pair_con, screened, amplitude, qmap):
    bf16, f32, i32 = jnp.bfloat16, jnp.float32, jnp.int32
    block = (2, 2, 16, 512)
    dma = pltpu.SemaphoreType.DMA
    hbm = pl.BlockSpec(memory_space=pl.ANY)
    vmem = pl.BlockSpec(memory_space=pltpu.VMEM)
    return pl.pallas_call(
        kernel,
        out_shape=jax.ShapeDtypeStruct((2, 16), f32),
        in_specs=[hbm] * 5,
        out_specs=vmem,
        scratch_shapes=[
            pltpu.VMEM((2, 16), bf16),
            pltpu.VMEM((2, 64), i32),
            pltpu.VMEM((2, 64, 16, 512), bf16),
            pltpu.VMEM((2, 64, 16, 512), bf16),
            pltpu.VMEM((2, 2048, 512), bf16),
            pltpu.VMEM((15, *block), bf16),
            pltpu.VMEM((15, *block), bf16),
            pltpu.VMEM((15, *block), bf16),
            pltpu.VMEM((16, *block), bf16),
            pltpu.VMEM((2, 2, 16, 2, *block), bf16),
            pltpu.VMEM((32, *block), bf16),
            pltpu.VMEM((16, *block), bf16),
            pltpu.VMEM((15, *block), bf16),
            pltpu.VMEM((2, 256, 512), f32),
            pltpu.VMEM((2, 1024, 256), bf16),
            pltpu.VMEM((2, 64), i32),
            pltpu.SMEM((2, 64), i32),
            pltpu.VMEM((32, 2, 128), f32),
            pltpu.VMEM((32, 2, 128), f32),
            pltpu.VMEM((128, 2, 128), f32),
            pltpu.SemaphoreType.REGULAR((3,)), dma((6,)), dma((16,)), dma((16,)), dma((3, 16)), dma((4, 16)), dma((32,)), dma((16,)), dma, dma((6,)),
            dma((2,)), dma((3,)), dma((3,)), dma((4,)), dma, dma((6,)),
        ],
        compiler_params=pltpu.CompilerParams(collective_id=0, has_side_effects=True),
    )(pair_con, pair_val, screened, amplitude, qmap)


def solution(mesh):
    placed = (
        P("blk", None, None, "ga"),
        P("blk", None, None, "ga"),
        P("blk", None, "ga"),
        P("blk", None),
        P("blk", None),
    )
    return jax.shard_map(
        body, mesh=mesh, in_specs=placed, out_specs=P("blk", None), check_vma=False
    )
```

```python
import jax
import jax.numpy as jnp
from jax import lax
from jax.experimental import pallas as pl
from jax.experimental.pallas import tpu as pltpu
from jax.sharding import PartitionSpec as P

MESH = pl.DeviceIdType.MESH
ORDER = ((2, 2), (1, 1), (3, 3), (1, 3), (3, 1), (2, 1), (1, 2), (2, 3), (3, 2), (2, 0), (0, 2), (0, 3), (1, 0), (3, 0), (0, 1), (0, 0))
HERE = 15
GROUPS = ((0, 4), (4, 4), (8, 4), (12, 2), (14, 1), (15, 1))
COLUMN = ((0, 1), (1, 1), (1, 0))


def iota(shape, dim):
    return lax.broadcasted_iota(jnp.int32, shape, dim)


def zero_one(cond):
    return jnp.where(cond, 1.0, 0.0).astype(jnp.bfloat16)


def kernel(
    con_hbm, val_hbm, w_hbm, amp_ref, qmap_hbm, out_ref,
    qmap_ref, con_raw, val_raw, w, s_send, d_send, vs_send, vd_send, con_all, val_all, transit, val_transit,
    acc, weight, rows_ref, partner, qa_all, part, gathered, fin, crossing,
    ready, load_sem, s_rs, d_rs, y_rs, p_rs, val_rs, vt_rs, qa_rs, home_rs, fin_rs,
    con_ss, val_ss, relay_ss, d2d_ss, qa_ss, home_ss, fin_ss,
):
    blk, ga = lax.axis_index("blk"), lax.axis_index("ga")
    lo, x, z = blk // 16, (blk // 4) % 4, blk % 4
    h, c = ga // 2, ga % 2

    def dev(dx, dz, flip_lo=0, flip_h=0, flip_c=0):
        to_lo = (lo + flip_lo) % 2
        to_h = (h + flip_h) % 2
        to_c = (c + flip_c) % 2
        return (to_lo * 16 + ((x + dx + 4) % 4) * 4 + (z + dz + 4) % 4, to_h * 2 + to_c)

    loads = [
        pltpu.make_async_copy(con_hbm, con_raw, load_sem.at[0]),
        pltpu.make_async_copy(val_hbm, val_raw, load_sem.at[1]),
        pltpu.make_async_copy(w_hbm, w, load_sem.at[2]),
        pltpu.make_async_copy(qmap_hbm, qmap_ref, load_sem.at[3]),
    ]
    along_x = [(d, 0, 0, 0, 0) for d in (2, 1, 3)]
    along_z = [(0, d, 0, 0, 0) for d in (2, 1, 3)]
    along_y = [(0, 0, 0, 1, 0), (0, 0, 1, 0, 0), (0, 0, 1, 1, 0)]
    other_core = [(0, 0, 0, 0, 1)]
    lines = along_y + along_x + along_z + other_core
    barrier = pltpu.get_barrier_semaphore()
    for offset in lines:
        pl.semaphore_signal(barrier, inc=1, device_id=dev(*offset), device_id_type=MESH)
    for n in (3, 1, 0):
        loads[n].start()

    def tell(group):
        for offset in group:
            pl.semaphore_signal(ready, inc=1, device_id=dev(*offset), device_id_type=MESH)

    def send(src, dst, ss, rs, to):
        pltpu.make_async_remote_copy(src, dst, ss, rs, device_id=to, device_id_type=MESH).start()

    def arrived(dst, rs):
        pltpu.make_async_copy(dst, dst, rs).wait()

    sent = arrived

    loads[3].wait()
    qmap = qmap_ref[...]
    for k in (0, 1):
        hit = qmap[k : k + 1, :] == iota((64, 64), 0)
        column = jnp.max(jnp.where(hit, iota((64, 64), 1), 0), axis=1, keepdims=True)
        square = jnp.where(iota((64, 64), 0) == iota((64, 64), 1), column, 0)
        rows_ref[k : k + 1, :] = jnp.max(square, axis=0, keepdims=True)
    to_smem = pltpu.make_async_copy(rows_ref, partner, load_sem.at[5])
    to_smem.start()
    place = zero_one(iota((16, 128), 0) + 64 == iota((16, 128), 1))
    moved = jnp.dot(amp_ref[...], place, preferred_element_type=jnp.float32)
    qa_all[blk] = moved + jnp.concatenate([qmap.astype(jnp.float32), jnp.zeros((2, 64), jnp.float32)], axis=1)
    to_smem.wait()

    def ordered(raw, k, q, dx, dz, fl):
        return raw[k, partner[k, dev(dx, dz, fl)[0] * 2 + q]]

    loads[1].wait()
    for fl, buffer in ((1, vd_send), (0, vs_send)):
        for t, (dx, dz) in enumerate(ORDER):
            for q in (0, 1):
                for k in (0, 1):
                    tile = ordered(val_raw, k, q, dx, dz, fl)
                    if t == HERE and not fl:
                        val_all[2 * HERE, q, k] = tile
                    else:
                        buffer[t, q, k] = tile
    pl.semaphore_wait(barrier, len(lines))
    tell(along_x + other_core)

    def val_along_y(t):
        if t == HERE:
            send(vd_send.at[t], val_all.at[2 * t + 1], val_ss.at[1], val_rs.at[2 * t + 1], dev(0, 0, 1))
        else:
            send(vd_send.at[t], val_transit.at[t], val_ss.at[1], vt_rs.at[t], dev(0, 0, 1))

    def val_onward(t):
        arrived(val_transit.at[t], vt_rs.at[t])
        send(val_transit.at[t], val_all.at[2 * t + 1], val_ss.at[2], val_rs.at[2 * t + 1], dev(*ORDER[t]))

    for t in range(15):
        val_along_y(t)
    loads[0].wait()
    for t, (dx, dz) in enumerate(ORDER):
        for fl, buffer in ((1, d_send), (0, s_send)):
            for q in (0, 1):
                for k in (0, 1):
                    tile = ordered(con_raw, k, q, dx, dz, fl)
                    if t != HERE:
                        buffer[t, q, k] = tile
                    elif fl:
                        transit[HERE, q, k] = tile
                    else:
                        con_all[0, 0, HERE, 0, q, k] = tile
    loads[2].start()
    pl.semaphore_wait(ready, 4)
    for block in range(0, 15, 4):
        for t in range(block, min(block + 4, 15)):
            send(d_send.at[t], transit.at[t], con_ss.at[0], d_rs.at[t], dev(*ORDER[t]))
        for t in range(block, min(block + 4, 15)):
            send(s_send.at[t], con_all.at[0, 0, t, 0], con_ss.at[1], s_rs.at[t], dev(*ORDER[t]))
        if block == 4:
            for t in range(15):
                send(qa_all.at[blk], qa_all.at[blk], qa_ss.at[0], qa_rs.at[0], dev(*ORDER[t]))
    for t in range(15):
        send(vs_send.at[t], val_all.at[2 * t], val_ss.at[0], val_rs.at[2 * t], dev(*ORDER[t]))
    def relay_d(t):
        if t != HERE:
            arrived(transit.at[t], d_rs.at[t])
        send(transit.at[t], con_all.at[0, 0, t, 1], relay_ss.at[0], y_rs.at[0, t], dev(0, 0, 1))
        send(transit.at[t], con_all.at[0, 1, t, 1], relay_ss.at[1], y_rs.at[1, t], dev(0, 0, 1, 1))

    def relay_s(t):
        here = con_all.at[0, 0, t, 0]
        if t != HERE:
            arrived(here, s_rs.at[t])
        send(here, con_all.at[0, 1, t, 0], relay_ss.at[2], y_rs.at[2, t], dev(0, 0, 0, 1))
        send(here, con_all.at[1, 0, t, 0], d2d_ss.at[3], p_rs.at[3, t], dev(0, 0, 0, 0, 1))

    def forward(t, n):
        gh, fl = COLUMN[n]
        arrived(con_all.at[0, gh, t, fl], y_rs.at[n, t])
        send(con_all.at[0, gh, t, fl], con_all.at[1, gh, t, fl], d2d_ss.at[n], p_rs.at[n, t], dev(0, 0, 0, 0, 1))

    def weights():
        arrived(qa_all.at[pl.ds(0, 16)], qa_rs.at[1])
        table = qa_all[...].reshape(64, 128)
        amps = table.astype(jnp.bfloat16)
        pick = zero_one(iota((128, 128), 0) == iota((128, 128), 1) + 64)
        amps = jnp.dot(amps, pick, preferred_element_type=jnp.float32).astype(jnp.bfloat16)
        row = iota((64, 64), 0)
        source = jnp.zeros((64, 64), jnp.int32)
        for t, (dx, dz) in enumerate(ORDER):
            for fl in (0, 1):
                source = jnp.where(row // 2 == t * 2 + fl, dev(-dx, -dz, fl)[0] * 2, source)
        perm = zero_one(source + row % 2 == iota((64, 64), 1))
        for q in (0, 1):
            mine = (blk * 2 + q).astype(jnp.float32)
            hot = zero_one(table[:, :64] == mine)
            chosen = jnp.dot(hot, amps, preferred_element_type=jnp.float32).astype(jnp.bfloat16)
            chosen = jnp.dot(perm, chosen, preferred_element_type=jnp.float32).astype(jnp.bfloat16)
            spread = zero_one(iota((256, 16), 0) // 16 == iota((256, 16), 1))
            columns = zero_one((iota((128, 256), 0) // 4 == iota((128, 256), 1) % 4) & (iota((128, 256), 0) < 16))
            for t0, n in GROUPS:
                rows = jnp.dot(spread[: 64 * n, : 4 * n], chosen[4 * t0 : 4 * (t0 + n)], preferred_element_type=jnp.float32)
                rows = jnp.where(iota((64 * n, 128), 0) % 4 == iota((64 * n, 128), 1) % 4, rows, 0.0).astype(jnp.bfloat16)
                full = jnp.dot(rows, columns, preferred_element_type=jnp.float32)
                same = iota((64 * n, 256), 0) // 16 == iota((64 * n, 256), 1) // 16
                weight[q, 64 * t0 : 64 * (t0 + n)] = jnp.where(same, full, 0.0).astype(jnp.bfloat16)

    def from_partner(t0, n, gh):
        for t in range(t0, t0 + n):
            for m, (of_h, fl) in enumerate(COLUMN + ((0, 0),)):
                if of_h == gh:
                    arrived(con_all.at[1, gh, t, fl], p_rs.at[m, t])

    def quarter(t0, n, gc, gh, first=False):
        g = ((h + gh) % 2) * 2 + (c + gc) % 2

        def one(q, carry):
            lhs = con_all[gc, gh, t0 : t0 + n, :, q].reshape(64 * n, 512)
            rhs = w[q, pl.ds(pl.multiple_of(g * 512, 512), 512), :]
            product = jnp.dot(lhs, rhs, preferred_element_type=jnp.float32)
            if first:
                acc[q, : 64 * n] = product
            else:
                acc[q, : 64 * n] += product
            return carry

        lax.fori_loop(0, 2, one, 0)

    def own(t0, n):
        quarter(t0, n, 0, 0, True)
        quarter(t0, n, 0, 1)

    def others(t0, n):
        for gh in (0, 1):
            from_partner(t0, n, gh)
            quarter(t0, n, 1, gh)

    def terms(t0, n):
        for t in range(t0, t0 + n):
            for fl in (0, 1):
                if t != HERE or fl:
                    arrived(val_all.at[t * 2 + fl], val_rs.at[t * 2 + fl])
        size = 64 * n
        total = jnp.zeros((size, size), jnp.float32)
        for q in (0, 1):
            vals = val_all[2 * t0 : 2 * (t0 + n), q].reshape(size, 512)
            unit = acc[q, :size].astype(jnp.bfloat16)
            full = lax.dot_general(unit, vals, (((1,), (1,)), ((), ())), preferred_element_type=jnp.float32)
            total = total + full * weight[q, 64 * t0 : 64 * (t0 + n), :size].astype(jnp.float32)
        lanes = iota((size, 128), 1)
        columns = zero_one(((iota((size, 128), 0) // 4) % 4 == lanes // 4) & (lanes < 16))
        high = total.astype(jnp.bfloat16)
        low = (total - high.astype(jnp.float32)).astype(jnp.bfloat16)
        summed = jnp.dot(high, columns, preferred_element_type=jnp.float32)
        summed = summed + jnp.dot(low, columns, preferred_element_type=jnp.float32)
        summed = jnp.where((iota((size, 128), 0) // 4) % 4 == lanes % 4, summed, 0.0)
        part[t0 : t0 + n] = jnp.sum(summed.reshape(4 * n, 16, 128), axis=1).reshape(n, 2, 2, 128)

    def home(t0, n):
        for t in range(t0, t0 + n):
            dx, dz = ORDER[t]
            send(part.at[t], gathered.at[t], home_ss, home_rs, dev(-dx, -dz))

    for t in range(15):
        relay_d(t)
        relay_s(t)
        val_onward(t)
        if t == 2:
            arrived(qa_all.at[pl.ds(0, 15)], qa_rs.at[0])
            plane = qa_all.at[pl.ds(lo * 16, 16)]
            send(plane, plane, qa_ss.at[1], qa_rs.at[1], dev(0, 0, 1))
    relay_s(HERE)
    relay_d(HERE)
    val_along_y(HERE)
    weights()
    loads[2].wait()
    for t in range(14):
        for n in range(3):
            forward(t, n)
        if t in (3, 7, 11):
            own(t - 3, 4)
        if t in (4, 8, 12):
            others(t - 4, 4)
            terms(t - 4, 4)
            home(t - 4, 4)
    own(12, 2)
    others(12, 2)
    terms(12, 2)
    home(12, 2)
    for n in range(3):
        forward(14, n)
    own(14, 1)
    others(14, 1)
    terms(14, 1)
    home(14, 1)
    forward(HERE, 1)
    forward(HERE, 2)
    quarter(HERE, 1, 0, 1, True)
    forward(HERE, 0)
    quarter(HERE, 1, 0, 0)
    from_partner(HERE, 1, 1)
    quarter(HERE, 1, 1, 1)
    from_partner(HERE, 1, 0)
    quarter(HERE, 1, 1, 0)
    terms(HERE, 1)
    arrived(gathered, home_rs)
    column = part[HERE] + jnp.sum(gathered[...], axis=0)
    fin[ga] = column[0]
    crossing[...] = column[1]
    for gh in (0, 1):
        for gc in (0, 1):
            send(crossing, fin.at[4 + ga], fin_ss, fin_rs, dev(0, 0, 1, gh, gc))
            if (gh, gc) != (0, 0):
                send(fin.at[ga], fin.at[ga], fin_ss, fin_rs, dev(0, 0, 0, gh, gc))
    arrived(fin.at[pl.ds(1, 7)], fin_rs)
    out_ref[...] = jnp.sum(fin[...], axis=0)[:, :16] / 64.0

    sent(d_send, con_ss.at[0])
    sent(s_send, con_ss.at[1])
    for n in range(3):
        sent(transit, relay_ss.at[n])
    for n in range(4):
        sent(transit, d2d_ss.at[n])
    sent(vs_send, val_ss.at[0])
    sent(vd_send, val_ss.at[1])
    sent(vs_send, val_ss.at[2])
    sent(qa_all.at[pl.ds(0, 15)], qa_ss.at[0])
    sent(qa_all.at[pl.ds(0, 16)], qa_ss.at[1])
    sent(gathered, home_ss)
    sent(fin.at[pl.ds(1, 7)], fin_ss)


def body(pair_val, pair_con, screened, amplitude, qmap):
    bf16, f32, i32 = jnp.bfloat16, jnp.float32, jnp.int32
    block = (2, 2, 16, 512)
    dma = pltpu.SemaphoreType.DMA
    hbm = pl.BlockSpec(memory_space=pl.ANY)
    vmem = pl.BlockSpec(memory_space=pltpu.VMEM)
    return pl.pallas_call(
        kernel,
        out_shape=jax.ShapeDtypeStruct((2, 16), f32),
        in_specs=[hbm, hbm, hbm, vmem, hbm],
        out_specs=vmem,
        scratch_shapes=[
            pltpu.VMEM((2, 64), i32),
            pltpu.VMEM((2, 64, 16, 512), bf16),
            pltpu.VMEM((2, 64, 16, 512), bf16),
            pltpu.VMEM((2, 2048, 512), bf16),
            pltpu.VMEM((15, *block), bf16),
            pltpu.VMEM((15, *block), bf16),
            pltpu.VMEM((15, *block), bf16),
            pltpu.VMEM((16, *block), bf16),
            pltpu.VMEM((2, 2, 16, 2, *block), bf16),
            pltpu.VMEM((32, *block), bf16),
            pltpu.VMEM((16, *block), bf16),
            pltpu.VMEM((15, *block), bf16),
            pltpu.VMEM((2, 256, 512), f32),
            pltpu.VMEM((2, 1024, 256), bf16),
            pltpu.VMEM((2, 64), i32),
            pltpu.SMEM((2, 64), i32),
            pltpu.VMEM((32, 2, 128), f32),
            pltpu.VMEM((16, 2, 2, 128), f32),
            pltpu.VMEM((15, 2, 2, 128), f32),
            pltpu.VMEM((8, 2, 128), f32),
            pltpu.VMEM((2, 128), f32),
            pltpu.SemaphoreType.REGULAR, dma((6,)), dma((16,)), dma((16,)), dma((3, 16)), dma((4, 16)), dma((32,)), dma((16,)), dma((2,)), dma, dma,
            dma((2,)), dma((3,)), dma((3,)), dma((4,)), dma((2,)), dma, dma,
        ],
        compiler_params=pltpu.CompilerParams(collective_id=0, has_side_effects=True, vmem_limit_bytes=55224 * 1024),
    )(pair_con, pair_val, screened, amplitude, qmap)


def solution(mesh):
    placed = (
        P("blk", None, None, "ga"),
        P("blk", None, None, "ga"),
        P("blk", None, "ga"),
        P("blk", None),
        P("blk", None),
    )
    return jax.shard_map(
        body, mesh=mesh, in_specs=placed, out_specs=P("blk", None), check_vma=False
    )
```

```python
import jax
import jax.numpy as jnp
from jax import lax
from jax.experimental import pallas as pl
from jax.experimental.pallas import tpu as pltpu
from jax.sharding import PartitionSpec as P

MESH = pl.DeviceIdType.MESH
ORDER = ((2, 2), (1, 1), (3, 3), (1, 3), (3, 1), (2, 1), (1, 2), (2, 3), (3, 2), (2, 0), (0, 2), (0, 3), (1, 0), (3, 0), (0, 1), (0, 0))
HERE = 15
GROUPS = ((0, 4), (4, 4), (8, 4), (12, 2), (14, 1), (15, 1))
Y_OF = (0, 0, 1, 1, 2, 2, 3, 3, 4, 4, 5, 5, 6, 7, 8, 9)
LO_OF = Y_OF[:15] + (10,)
PARTNER_OF = ((0, 0),) * 4 + ((1, 1),) * 4 + ((2, 2),) * 4 + ((3, 3),) * 2 + ((4, 4),) + ((5, 6),)


def group_of(t):
    return [t0 <= t < t0 + n for t0, n in GROUPS].index(True)


def iota(shape, dim):
    return lax.broadcasted_iota(jnp.int32, shape, dim)


def zero_one(cond):
    return jnp.where(cond, 1.0, 0.0).astype(jnp.bfloat16)


def kernel(
    con_hbm, val_hbm, w_hbm, amp_ref, qmap_hbm, out_ref,
    qmap_ref, con_raw, val_raw, w, s_send, d_send, vs_send, vd_send, con_all, val_all, transit, val_transit,
    acc, weight, rows_ref, partner, qa_all, part, gathered, fin, crossing,
    ready, load_sem, con_rs, y_rs, p_rs, val_rs, vt_rs, qa_rs, home_rs, fin_rs,
    con_ss, vd_ss, val_ss, relay_ss, d2d_ss, qa_ss, home_ss, fin_ss,
):
    blk, ga = lax.axis_index("blk"), lax.axis_index("ga")
    lo, x, z = blk // 16, (blk // 4) % 4, blk % 4
    h, c = ga // 2, ga % 2

    def dev(dx, dz, flip_lo=0, flip_h=0, flip_c=0):
        to_lo = (lo + flip_lo) % 2
        to_h = (h + flip_h) % 2
        to_c = (c + flip_c) % 2
        return (to_lo * 16 + ((x + dx + 4) % 4) * 4 + (z + dz + 4) % 4, to_h * 2 + to_c)

    loads = [
        pltpu.make_async_copy(con_hbm, con_raw, load_sem.at[0]),
        pltpu.make_async_copy(val_hbm, val_raw, load_sem.at[1]),
        pltpu.make_async_copy(w_hbm, w, load_sem.at[1]),
        pltpu.make_async_copy(qmap_hbm, qmap_ref, load_sem.at[2]),
    ]
    along_x = [(d, 0, 0, 0, 0) for d in (2, 1, 3)]
    along_z = [(0, d, 0, 0, 0) for d in (2, 1, 3)]
    along_y = [(0, 0, 0, 1, 0), (0, 0, 1, 0, 0), (0, 0, 1, 1, 0)]
    other_core = [(0, 0, 0, 0, 1)]
    lines = along_y + along_x + along_z + other_core
    barrier = pltpu.get_barrier_semaphore()
    for offset in lines:
        pl.semaphore_signal(barrier, inc=1, device_id=dev(*offset), device_id_type=MESH)
    for n in (3, 1, 0):
        loads[n].start()

    def tell(group):
        for offset in group:
            pl.semaphore_signal(ready, inc=1, device_id=dev(*offset), device_id_type=MESH)

    def send(src, dst, ss, rs, to):
        pltpu.make_async_remote_copy(src, dst, ss, rs, device_id=to, device_id_type=MESH).start()

    def arrived(dst, rs):
        pltpu.make_async_copy(dst, dst, rs).wait()

    sent = arrived

    loads[3].wait()
    qmap = qmap_ref[...]
    for k in (0, 1):
        hit = qmap[k : k + 1, :] == iota((64, 64), 0)
        column = jnp.max(jnp.where(hit, iota((64, 64), 1), 0), axis=1, keepdims=True)
        square = jnp.where(iota((64, 64), 0) == iota((64, 64), 1), column, 0)
        rows_ref[k : k + 1, :] = jnp.max(square, axis=0, keepdims=True)
    to_smem = pltpu.make_async_copy(rows_ref, partner, load_sem.at[2])
    to_smem.start()
    place = zero_one(iota((16, 128), 0) + 64 == iota((16, 128), 1))
    moved = jnp.dot(amp_ref[...], place, preferred_element_type=jnp.float32)
    qa_all[blk] = moved + jnp.concatenate([qmap.astype(jnp.float32), jnp.zeros((2, 64), jnp.float32)], axis=1)
    to_smem.wait()

    def ordered(raw, k, q, dx, dz, fl):
        return raw[k, partner[k, dev(dx, dz, fl)[0] * 2 + q]]

    loads[1].wait()
    for fl, buffer in ((1, vd_send), (0, vs_send)):
        for t, (dx, dz) in enumerate(ORDER):
            for q in (0, 1):
                for k in (0, 1):
                    tile = ordered(val_raw, k, q, dx, dz, fl)
                    if t == HERE and not fl:
                        val_all[2 * HERE, q, k] = tile
                    else:
                        buffer[t, q, k] = tile
    pl.semaphore_wait(barrier, len(lines))
    tell(along_x + other_core)

    def val_along_y(t):
        some = pl.ds(t, 3)
        send(vd_send.at[some], val_transit.at[some], vd_ss, vt_rs.at[t // 3], dev(0, 0, 1))

    def val_onward(t):
        some = pl.ds(t, 3)
        arrived(val_transit.at[some], vt_rs.at[t // 3])
        for u in range(t, t + 3):
            send(val_transit.at[u], val_all.at[2 * u + 1], val_ss, val_rs.at[group_of(u)], dev(*ORDER[u]))

    for t in range(0, 15, 3):
        val_along_y(t)
    loads[0].wait()
    for t, (dx, dz) in enumerate(ORDER):
        for fl, buffer in ((1, d_send), (0, s_send)):
            for q in (0, 1):
                for k in (0, 1):
                    tile = ordered(con_raw, k, q, dx, dz, fl)
                    if t != HERE:
                        buffer[t, q, k] = tile
                    elif fl:
                        transit[HERE, q, k] = tile
                    else:
                        con_all[0, 0, HERE, 0, q, k] = tile
    loads[2].start()
    pl.semaphore_wait(ready, 4)
    for t in range(15):
        send(qa_all.at[blk], qa_all.at[blk], qa_ss, qa_rs.at[0], dev(*ORDER[t]))
    for block in range(0, 15, 4):
        for t in range(block, min(block + 4, 15)):
            send(d_send.at[t], transit.at[t], con_ss, con_rs.at[t // 2], dev(*ORDER[t]))
        for t in range(block, min(block + 4, 15)):
            send(s_send.at[t], con_all.at[0, 0, t, 0], con_ss, con_rs.at[t // 2], dev(*ORDER[t]))
    for t in range(15):
        send(vs_send.at[t], val_all.at[2 * t], val_ss, val_rs.at[group_of(t)], dev(*ORDER[t]))

    def relay(t):
        send(transit.at[t], con_all.at[0, 0, t, 1], relay_ss, y_rs.at[LO_OF[t]], dev(0, 0, 1))
        send(transit.at[t], con_all.at[0, 1, t, 1], relay_ss, y_rs.at[Y_OF[t]], dev(0, 0, 1, 1))
        send(con_all.at[0, 0, t, 0], con_all.at[0, 1, t, 0], relay_ss, y_rs.at[Y_OF[t]], dev(0, 0, 0, 1))

    def forward(t, n, gh):
        some = con_all.at[0, gh, pl.ds(t, n)]
        send(some, con_all.at[1, gh, pl.ds(t, n)], d2d_ss, p_rs.at[PARTNER_OF[t][gh]], dev(0, 0, 0, 0, 1))

    def come(t, n):
        arrived(val_all.at[pl.ds(0, 3 * n)], y_rs.at[Y_OF[t]])
        for gh in (0, 1):
            forward(t, n, gh)

    def weights():
        arrived(qa_all.at[pl.ds(0, 16)], qa_rs.at[1])
        table = qa_all[...].reshape(64, 128)
        amps = table.astype(jnp.bfloat16)
        pick = zero_one(iota((128, 128), 0) == iota((128, 128), 1) + 64)
        amps = jnp.dot(amps, pick, preferred_element_type=jnp.float32).astype(jnp.bfloat16)
        row = iota((64, 64), 0)
        source = jnp.zeros((64, 64), jnp.int32)
        for t, (dx, dz) in enumerate(ORDER):
            for fl in (0, 1):
                source = jnp.where(row // 2 == t * 2 + fl, dev(-dx, -dz, fl)[0] * 2, source)
        perm = zero_one(source + row % 2 == iota((64, 64), 1))
        for q in (0, 1):
            mine = (blk * 2 + q).astype(jnp.float32)
            hot = zero_one(table[:, :64] == mine)
            chosen = jnp.dot(hot, amps, preferred_element_type=jnp.float32).astype(jnp.bfloat16)
            chosen = jnp.dot(perm, chosen, preferred_element_type=jnp.float32).astype(jnp.bfloat16)
            spread = zero_one(iota((256, 16), 0) // 16 == iota((256, 16), 1))
            columns = zero_one((iota((128, 256), 0) // 4 == iota((128, 256), 1) % 4) & (iota((128, 256), 0) < 16))
            for t0, n in GROUPS:
                rows = jnp.dot(spread[: 64 * n, : 4 * n], chosen[4 * t0 : 4 * (t0 + n)], preferred_element_type=jnp.float32)
                rows = jnp.where(iota((64 * n, 128), 0) % 4 == iota((64 * n, 128), 1) % 4, rows, 0.0).astype(jnp.bfloat16)
                full = jnp.dot(rows, columns, preferred_element_type=jnp.float32)
                same = iota((64 * n, 256), 0) // 16 == iota((64 * n, 256), 1) // 16
                weight[q, 64 * t0 : 64 * (t0 + n)] = jnp.where(same, full, 0.0).astype(jnp.bfloat16)

    def quarter(t0, n, gc, gh, first=False):
        g = ((h + gh) % 2) * 2 + (c + gc) % 2

        def one(q, carry):
            lhs = con_all[gc, gh, t0 : t0 + n, :, q].reshape(64 * n, 512)
            rhs = w[q, pl.ds(pl.multiple_of(g * 512, 512), 512), :]
            product = jnp.dot(lhs, rhs, preferred_element_type=jnp.float32)
            if first:
                acc[q, : 64 * n] = product
            else:
                acc[q, : 64 * n] += product
            return carry

        lax.fori_loop(0, 2, one, 0)

    def own(t0, n):
        quarter(t0, n, 0, 0, True)
        quarter(t0, n, 0, 1)

    def others(t0, n):
        arrived(con_all.at[1, :, pl.ds(t0, n)], p_rs.at[PARTNER_OF[t0][0]])
        quarter(t0, n, 1, 0)
        quarter(t0, n, 1, 1)

    def terms(t0, n):
        first = 2 * t0 + (t0 == HERE)
        some = pl.ds(first, 2 * (t0 + n) - first)
        arrived(val_all.at[some], val_rs.at[group_of(t0)])
        size = 64 * n
        total = jnp.zeros((size, size), jnp.float32)
        for q in (0, 1):
            vals = val_all[2 * t0 : 2 * (t0 + n), q].reshape(size, 512)
            unit = acc[q, :size].astype(jnp.bfloat16)
            full = lax.dot_general(unit, vals, (((1,), (1,)), ((), ())), preferred_element_type=jnp.float32)
            total = total + full * weight[q, 64 * t0 : 64 * (t0 + n), :size].astype(jnp.float32)
        lanes = iota((size, 128), 1)
        columns = zero_one(((iota((size, 128), 0) // 4) % 4 == lanes // 4) & (lanes < 16))
        high = total.astype(jnp.bfloat16)
        low = (total - high.astype(jnp.float32)).astype(jnp.bfloat16)
        summed = jnp.dot(high, columns, preferred_element_type=jnp.float32)
        summed = summed + jnp.dot(low, columns, preferred_element_type=jnp.float32)
        summed = jnp.where((iota((size, 128), 0) // 4) % 4 == lanes % 4, summed, 0.0)
        part[t0 : t0 + n] = jnp.sum(summed.reshape(4 * n, 16, 128), axis=1).reshape(n, 2, 2, 128)

    def home(t0, n):
        for t in range(t0, t0 + n):
            dx, dz = ORDER[t]
            send(part.at[t], gathered.at[t], home_ss, home_rs, dev(-dx, -dz))

    for t in range(15):
        if t % 2 == 0:
            n = min(2, 15 - t)
            arrived(con_all.at[0, 0, pl.ds(t, n)], con_rs.at[t // 2])
        relay(t)
        if t == 3:
            arrived(qa_all.at[pl.ds(0, 15)], qa_rs.at[0])
            plane = qa_all.at[pl.ds(lo * 16, 16)]
            send(plane, plane, qa_ss, qa_rs.at[1], dev(0, 0, 1))
        if t % 3 == 2:
            val_onward(t - 2)
    weights()
    loads[2].wait()
    for t in range(0, 14, 2):
        if t < 12:
            come(t, 2)
        else:
            come(12, 1)
        if t in (4, 8, 12):
            others(t - 4, 4)
            terms(t - 4, 4)
            home(t - 4, 4)
        if t in (2, 6, 10):
            own(t - 2, 4)
    come(13, 1)
    relay(HERE)
    send(vd_send.at[HERE], val_all.at[2 * HERE + 1], vd_ss, val_rs.at[group_of(HERE)], dev(0, 0, 1))
    own(12, 2)
    others(12, 2)
    terms(12, 2)
    home(12, 2)
    come(14, 1)
    own(14, 1)
    others(14, 1)
    terms(14, 1)
    home(14, 1)
    arrived(con_all.at[0, 1, HERE], y_rs.at[Y_OF[HERE]])
    forward(HERE, 1, 1)
    quarter(HERE, 1, 0, 1, True)
    arrived(con_all.at[0, 0, HERE, 1], y_rs.at[LO_OF[HERE]])
    forward(HERE, 1, 0)
    quarter(HERE, 1, 0, 0)
    arrived(con_all.at[1, 1, HERE], p_rs.at[PARTNER_OF[HERE][1]])
    quarter(HERE, 1, 1, 1)
    arrived(con_all.at[1, 0, HERE], p_rs.at[PARTNER_OF[HERE][0]])
    quarter(HERE, 1, 1, 0)
    terms(HERE, 1)
    arrived(gathered, home_rs)
    column = part[HERE] + jnp.sum(gathered[...], axis=0)
    fin[ga] = column[0]
    crossing[...] = column[1]
    for gh in (0, 1):
        for gc in (0, 1):
            send(crossing, fin.at[4 + ga], fin_ss, fin_rs, dev(0, 0, 1, gh, gc))
            if (gh, gc) != (0, 0):
                send(fin.at[ga], fin.at[ga], fin_ss, fin_rs, dev(0, 0, 0, gh, gc))
    arrived(fin.at[pl.ds(1, 7)], fin_rs)
    out_ref[...] = jnp.sum(fin[...], axis=0)[:, :16] / 64.0

    sent(val_all.at[pl.ds(0, 30)], con_ss)
    sent(con_all.at[0, :, pl.ds(0, 12)], relay_ss)
    sent(con_all.at[0], d2d_ss)
    sent(vd_send, vd_ss)
    sent(val_all.at[pl.ds(0, 30)], val_ss)
    sent(qa_all.at[pl.ds(0, 31)], qa_ss)
    sent(gathered, home_ss)
    sent(fin.at[pl.ds(1, 7)], fin_ss)


def body(pair_val, pair_con, screened, amplitude, qmap):
    bf16, f32, i32 = jnp.bfloat16, jnp.float32, jnp.int32
    block = (2, 2, 16, 512)
    dma = pltpu.SemaphoreType.DMA
    hbm = pl.BlockSpec(memory_space=pl.ANY)
    vmem = pl.BlockSpec(memory_space=pltpu.VMEM)
    return pl.pallas_call(
        kernel,
        out_shape=jax.ShapeDtypeStruct((2, 16), f32),
        in_specs=[hbm, hbm, hbm, vmem, hbm],
        out_specs=vmem,
        scratch_shapes=[
            pltpu.VMEM((2, 64), i32),
            pltpu.VMEM((2, 64, 16, 512), bf16),
            pltpu.VMEM((2, 64, 16, 512), bf16),
            pltpu.VMEM((2, 2048, 512), bf16),
            pltpu.VMEM((15, *block), bf16),
            pltpu.VMEM((15, *block), bf16),
            pltpu.VMEM((15, *block), bf16),
            pltpu.VMEM((16, *block), bf16),
            pltpu.VMEM((2, 2, 16, 2, *block), bf16),
            pltpu.VMEM((32, *block), bf16),
            pltpu.VMEM((16, *block), bf16),
            pltpu.VMEM((15, *block), bf16),
            pltpu.VMEM((2, 256, 512), f32),
            pltpu.VMEM((2, 1024, 256), bf16),
            pltpu.VMEM((2, 64), i32),
            pltpu.SMEM((2, 64), i32),
            pltpu.VMEM((32, 2, 128), f32),
            pltpu.VMEM((16, 2, 2, 128), f32),
            pltpu.VMEM((15, 2, 2, 128), f32),
            pltpu.VMEM((8, 2, 128), f32),
            pltpu.VMEM((2, 128), f32),
            pltpu.SemaphoreType.REGULAR, dma((3,)), dma((8,)), dma((11,)), dma((7,)), dma((6,)), dma((5,)), dma((2,)), dma, dma,
            dma, dma, dma, dma, dma, dma, dma, dma,
        ],
        compiler_params=pltpu.CompilerParams(collective_id=0, has_side_effects=True, vmem_limit_bytes=55224 * 1024),
    )(pair_con, pair_val, screened, amplitude, qmap)


def solution(mesh):
    placed = (
        P("blk", None, None, "ga"),
        P("blk", None, None, "ga"),
        P("blk", None, "ga"),
        P("blk", None),
        P("blk", None),
    )
    return jax.shard_map(
        body, mesh=mesh, in_specs=placed, out_specs=P("blk", None), check_vma=False
    )
```

```python
import jax
import jax.numpy as jnp
from jax import lax
from jax.experimental import pallas as pl
from jax.experimental.pallas import tpu as pltpu
from jax.sharding import PartitionSpec as P

MESH = pl.DeviceIdType.MESH
ORDER = ((2, 2), (1, 1), (3, 3), (1, 3), (3, 1), (2, 1), (1, 2), (2, 3), (3, 2), (2, 0), (0, 2), (0, 3), (1, 0), (3, 0), (0, 1), (0, 0))
HERE = 15
GROUPS = ((0, 4), (4, 4), (8, 4), (12, 2), (14, 1), (15, 1))
Y_OF = (0, 0, 1, 1, 2, 2, 3, 3, 4, 4, 5, 5, 6, 7, 8, 9)
LO_OF = Y_OF[:14] + (11, 10)
PARTNER_OF = ((0, 0),) * 4 + ((1, 1),) * 4 + ((2, 2),) * 4 + ((3, 3),) * 2 + ((4, 7),) + ((5, 6),)


def group_of(t):
    return [t0 <= t < t0 + n for t0, n in GROUPS].index(True)


def iota(shape, dim):
    return lax.broadcasted_iota(jnp.int32, shape, dim)


def zero_one(cond):
    return jnp.where(cond, 1.0, 0.0).astype(jnp.bfloat16)


def kernel(
    con_hbm, val_hbm, w_hbm, amp_ref, qmap_hbm, out_ref,
    qmap_ref, con_raw, val_raw, w, s_send, d_send, vs_send, vd_send, con_all, val_all, transit, val_transit,
    acc, weight, rows_ref, partner, qa_all, part, gathered, fin, crossing,
    ready, load_sem, con_rs, y_rs, p_rs, val_rs, vt_rs, qa_rs, home_rs, fin_rs,
    con_ss, vd_ss, val_ss, relay_ss, d2d_ss, qa_ss, home_ss, fin_ss,
):
    blk, ga = lax.axis_index("blk"), lax.axis_index("ga")
    lo, x, z = blk // 16, (blk // 4) % 4, blk % 4
    h, c = ga // 2, ga % 2

    def dev(dx, dz, flip_lo=0, flip_h=0, flip_c=0):
        to_lo = (lo + flip_lo) % 2
        to_h = (h + flip_h) % 2
        to_c = (c + flip_c) % 2
        return (to_lo * 16 + ((x + dx + 4) % 4) * 4 + (z + dz + 4) % 4, to_h * 2 + to_c)

    loads = [
        pltpu.make_async_copy(con_hbm, con_raw, load_sem.at[0]),
        pltpu.make_async_copy(val_hbm, val_raw, load_sem.at[1]),
        pltpu.make_async_copy(w_hbm, w, load_sem.at[1]),
        pltpu.make_async_copy(qmap_hbm, qmap_ref, load_sem.at[2]),
    ]
    near = [(0, 0, 1, 0, 0), (0, 0, 1, 1, 0), (0, 0, 0, 0, 1), (1, 0, 0, 0, 0), (3, 0, 0, 0, 0), (0, 1, 0, 0, 0), (0, 3, 0, 0, 0)]
    along_x = [(d, 0, 0, 0, 0) for d in (2, 1, 3)]
    other_core = [(0, 0, 0, 0, 1)]
    barrier = pltpu.get_barrier_semaphore()
    for offset in near:
        pl.semaphore_signal(barrier, inc=1, device_id=dev(*offset), device_id_type=MESH)
    for n in (3, 1, 0):
        loads[n].start()

    def tell(stage, group):
        for offset in group:
            pl.semaphore_signal(ready.at[stage], inc=1, device_id=dev(*offset), device_id_type=MESH)

    def send(src, dst, ss, rs, to):
        pltpu.make_async_remote_copy(src, dst, ss, rs, device_id=to, device_id_type=MESH).start()

    def arrived(dst, rs):
        pltpu.make_async_copy(dst, dst, rs).wait()

    sent = arrived

    loads[3].wait()
    qmap = qmap_ref[...]
    for k in (0, 1):
        hit = qmap[k : k + 1, :] == iota((64, 64), 0)
        column = jnp.max(jnp.where(hit, iota((64, 64), 1), 0), axis=1, keepdims=True)
        square = jnp.where(iota((64, 64), 0) == iota((64, 64), 1), column, 0)
        rows_ref[k : k + 1, :] = jnp.max(square, axis=0, keepdims=True)
    to_smem = pltpu.make_async_copy(rows_ref, partner, load_sem.at[2])
    to_smem.start()
    place = zero_one(iota((16, 128), 0) + 64 == iota((16, 128), 1))
    moved = jnp.dot(amp_ref[...], place, preferred_element_type=jnp.float32)
    qa_all[blk] = moved + jnp.concatenate([qmap.astype(jnp.float32), jnp.zeros((2, 64), jnp.float32)], axis=1)
    to_smem.wait()

    def ordered(raw, k, q, dx, dz, fl):
        return raw[k, partner[k, dev(dx, dz, fl)[0] * 2 + q]]

    loads[1].wait()
    for fl, buffer in ((1, vd_send), (0, vs_send)):
        for t, (dx, dz) in enumerate(ORDER):
            for q in (0, 1):
                for k in (0, 1):
                    tile = ordered(val_raw, k, q, dx, dz, fl)
                    if t == HERE and not fl:
                        val_all[2 * HERE, q, k] = tile
                    else:
                        buffer[t, q, k] = tile
    pl.semaphore_wait(barrier, len(near))
    tell(0, near)

    def val_along_y(t):
        some = pl.ds(t, 3)
        send(vd_send.at[some], val_transit.at[some], vd_ss, vt_rs.at[t // 3], dev(0, 0, 1))

    def val_onward(t):
        some = pl.ds(t, 3)
        arrived(val_transit.at[some], vt_rs.at[t // 3])
        for u in range(t, t + 3):
            send(val_transit.at[u], val_all.at[2 * u + 1], val_ss, val_rs.at[group_of(u)], dev(*ORDER[u]))

    for t in range(0, 15, 3):
        val_along_y(t)
    loads[0].wait()
    for t, (dx, dz) in enumerate(ORDER):
        for fl, buffer in ((1, d_send), (0, s_send)):
            for q in (0, 1):
                for k in (0, 1):
                    tile = ordered(con_raw, k, q, dx, dz, fl)
                    if t != HERE:
                        buffer[t, q, k] = tile
                    elif fl:
                        transit[HERE, q, k] = tile
                    else:
                        con_all[0, 0, HERE, 0, q, k] = tile
    loads[2].start()
    pl.semaphore_wait(ready.at[0], len(near))
    tell(1, along_x + other_core)
    pl.semaphore_wait(ready.at[1], 4)
    for t in range(15):
        send(qa_all.at[blk], qa_all.at[blk], qa_ss, qa_rs.at[0], dev(*ORDER[t]))
    for block in range(0, 15, 4):
        for t in range(block, min(block + 4, 15)):
            send(d_send.at[t], transit.at[t], con_ss, con_rs.at[t // 2], dev(*ORDER[t]))
        for t in range(block, min(block + 4, 15)):
            send(s_send.at[t], con_all.at[0, 0, t, 0], con_ss, con_rs.at[t // 2], dev(*ORDER[t]))
    for t in range(15):
        send(vs_send.at[t], val_all.at[2 * t], val_ss, val_rs.at[group_of(t)], dev(*ORDER[t]))

    def relay(t):
        send(transit.at[t], con_all.at[0, 0, t, 1], relay_ss, y_rs.at[LO_OF[t]], dev(0, 0, 1))
        send(transit.at[t], con_all.at[0, 1, t, 1], relay_ss, y_rs.at[Y_OF[t]], dev(0, 0, 1, 1))
        send(con_all.at[0, 0, t, 0], con_all.at[0, 1, t, 0], relay_ss, y_rs.at[Y_OF[t]], dev(0, 0, 0, 1))

    def forward(t, n, gh):
        some = con_all.at[0, gh, pl.ds(t, n)]
        send(some, con_all.at[1, gh, pl.ds(t, n)], d2d_ss, p_rs.at[PARTNER_OF[t][gh]], dev(0, 0, 0, 0, 1))

    def come(t, n):
        arrived(val_all.at[pl.ds(0, 3 * n)], y_rs.at[Y_OF[t]])
        for gh in (0, 1):
            forward(t, n, gh)

    def weights():
        arrived(qa_all.at[pl.ds(0, 16)], qa_rs.at[1])
        table = qa_all[...].reshape(64, 128)
        amps = table.astype(jnp.bfloat16)
        pick = zero_one(iota((128, 128), 0) == iota((128, 128), 1) + 64)
        amps = jnp.dot(amps, pick, preferred_element_type=jnp.float32).astype(jnp.bfloat16)
        row = iota((64, 64), 0)
        source = jnp.zeros((64, 64), jnp.int32)
        for t, (dx, dz) in enumerate(ORDER):
            for fl in (0, 1):
                source = jnp.where(row // 2 == t * 2 + fl, dev(-dx, -dz, fl)[0] * 2, source)
        perm = zero_one(source + row % 2 == iota((64, 64), 1))
        for q in (0, 1):
            mine = (blk * 2 + q).astype(jnp.float32)
            hot = zero_one(table[:, :64] == mine)
            chosen = jnp.dot(hot, amps, preferred_element_type=jnp.float32).astype(jnp.bfloat16)
            chosen = jnp.dot(perm, chosen, preferred_element_type=jnp.float32).astype(jnp.bfloat16)
            spread = zero_one(iota((256, 16), 0) // 16 == iota((256, 16), 1))
            columns = zero_one((iota((128, 256), 0) // 4 == iota((128, 256), 1) % 4) & (iota((128, 256), 0) < 16))
            for t0, n in GROUPS:
                rows = jnp.dot(spread[: 64 * n, : 4 * n], chosen[4 * t0 : 4 * (t0 + n)], preferred_element_type=jnp.float32)
                rows = jnp.where(iota((64 * n, 128), 0) % 4 == iota((64 * n, 128), 1) % 4, rows, 0.0).astype(jnp.bfloat16)
                full = jnp.dot(rows, columns, preferred_element_type=jnp.float32)
                same = iota((64 * n, 256), 0) // 16 == iota((64 * n, 256), 1) // 16
                weight[q, 64 * t0 : 64 * (t0 + n)] = jnp.where(same, full, 0.0).astype(jnp.bfloat16)

    def quarter(t0, n, gc, gh, first=False):
        g = ((h + gh) % 2) * 2 + (c + gc) % 2

        def one(q, carry):
            lhs = con_all[gc, gh, t0 : t0 + n, :, q].reshape(64 * n, 512)
            rhs = w[q, pl.ds(pl.multiple_of(g * 512, 512), 512), :]
            product = jnp.dot(lhs, rhs, preferred_element_type=jnp.float32)
            if first:
                acc[q, : 64 * n] = product
            else:
                acc[q, : 64 * n] += product
            return carry

        lax.fori_loop(0, 2, one, 0)

    def own(t0, n):
        quarter(t0, n, 0, 0, True)
        quarter(t0, n, 0, 1)

    def others(t0, n):
        arrived(con_all.at[1, :, pl.ds(t0, n)], p_rs.at[PARTNER_OF[t0][0]])
        quarter(t0, n, 1, 0)
        quarter(t0, n, 1, 1)

    def terms(t0, n):
        first = 2 * t0 + (t0 == HERE)
        some = pl.ds(first, 2 * (t0 + n) - first)
        arrived(val_all.at[some], val_rs.at[group_of(t0)])
        size = 64 * n
        total = jnp.zeros((size, size), jnp.float32)
        for q in (0, 1):
            vals = val_all[2 * t0 : 2 * (t0 + n), q].reshape(size, 512)
            unit = acc[q, :size].astype(jnp.bfloat16)
            full = lax.dot_general(unit, vals, (((1,), (1,)), ((), ())), preferred_element_type=jnp.float32)
            total = total + full * weight[q, 64 * t0 : 64 * (t0 + n), :size].astype(jnp.float32)
        lanes = iota((size, 128), 1)
        columns = zero_one(((iota((size, 128), 0) // 4) % 4 == lanes // 4) & (lanes < 16))
        high = total.astype(jnp.bfloat16)
        low = (total - high.astype(jnp.float32)).astype(jnp.bfloat16)
        summed = jnp.dot(high, columns, preferred_element_type=jnp.float32)
        summed = summed + jnp.dot(low, columns, preferred_element_type=jnp.float32)
        summed = jnp.where((iota((size, 128), 0) // 4) % 4 == lanes % 4, summed, 0.0)
        part[t0 : t0 + n] = jnp.sum(summed.reshape(4 * n, 16, 128), axis=1).reshape(n, 2, 2, 128)

    def home(t0, n):
        for t in range(t0, t0 + n):
            dx, dz = ORDER[t]
            send(part.at[t], gathered.at[t], home_ss, home_rs, dev(-dx, -dz))

    for t in range(15):
        if t % 2 == 0:
            n = min(2, 15 - t)
            arrived(con_all.at[0, 0, pl.ds(t, n)], con_rs.at[t // 2])
        relay(t)
        if t == 3:
            arrived(qa_all.at[pl.ds(0, 15)], qa_rs.at[0])
            plane = qa_all.at[pl.ds(lo * 16, 16)]
            send(plane, plane, qa_ss, qa_rs.at[1], dev(0, 0, 1))
        if t % 3 == 2:
            val_onward(t - 2)
    weights()
    loads[2].wait()
    for t in range(0, 14, 2):
        if t < 12:
            come(t, 2)
        else:
            come(12, 1)
        if t in (4, 8, 12):
            others(t - 4, 4)
            terms(t - 4, 4)
            home(t - 4, 4)
        if t in (2, 6, 10):
            own(t - 2, 4)
    come(13, 1)
    relay(HERE)
    send(vd_send.at[HERE], val_all.at[2 * HERE + 1], vd_ss, val_rs.at[group_of(HERE)], dev(0, 0, 1))
    own(12, 2)
    others(12, 2)
    terms(12, 2)
    home(12, 2)
    for t in (14, HERE):
        arrived(con_all.at[0, 0, t, 1], y_rs.at[LO_OF[t]])
        forward(t, 1, 0)
        quarter(t, 1, 0, 0, True)
        arrived(con_all.at[0, 1, t], y_rs.at[Y_OF[t]])
        forward(t, 1, 1)
        quarter(t, 1, 0, 1)
        arrived(con_all.at[1, 0, t], p_rs.at[PARTNER_OF[t][0]])
        quarter(t, 1, 1, 0)
        arrived(con_all.at[1, 1, t], p_rs.at[PARTNER_OF[t][1]])
        quarter(t, 1, 1, 1)
        if t == 14:
            terms(14, 1)
            home(14, 1)
    terms(HERE, 1)
    arrived(gathered, home_rs)
    column = part[HERE] + jnp.sum(gathered[...], axis=0)
    fin[ga] = column[0]
    crossing[...] = column[1]
    for gh in (0, 1):
        for gc in (0, 1):
            send(crossing, fin.at[4 + ga], fin_ss, fin_rs, dev(0, 0, 1, gh, gc))
            if (gh, gc) != (0, 0):
                send(fin.at[ga], fin.at[ga], fin_ss, fin_rs, dev(0, 0, 0, gh, gc))
    arrived(fin.at[pl.ds(1, 7)], fin_rs)
    out_ref[...] = jnp.sum(fin[...], axis=0)[:, :16] / 64.0

    sent(val_all.at[pl.ds(0, 30)], con_ss)
    sent(con_all.at[0, :, pl.ds(0, 12)], relay_ss)
    sent(con_all.at[0], d2d_ss)
    sent(vd_send, vd_ss)
    sent(val_all.at[pl.ds(0, 30)], val_ss)
    sent(qa_all.at[pl.ds(0, 31)], qa_ss)
    sent(gathered, home_ss)
    sent(fin.at[pl.ds(1, 7)], fin_ss)


def body(pair_val, pair_con, screened, amplitude, qmap):
    bf16, f32, i32 = jnp.bfloat16, jnp.float32, jnp.int32
    block = (2, 2, 16, 512)
    dma = pltpu.SemaphoreType.DMA
    hbm = pl.BlockSpec(memory_space=pl.ANY)
    vmem = pl.BlockSpec(memory_space=pltpu.VMEM)
    return pl.pallas_call(
        kernel,
        out_shape=jax.ShapeDtypeStruct((2, 16), f32),
        in_specs=[hbm, hbm, hbm, vmem, hbm],
        out_specs=vmem,
        scratch_shapes=[
            pltpu.VMEM((2, 64), i32),
            pltpu.VMEM((2, 64, 16, 512), bf16),
            pltpu.VMEM((2, 64, 16, 512), bf16),
            pltpu.VMEM((2, 2048, 512), bf16),
            pltpu.VMEM((15, *block), bf16),
            pltpu.VMEM((15, *block), bf16),
            pltpu.VMEM((15, *block), bf16),
            pltpu.VMEM((16, *block), bf16),
            pltpu.VMEM((2, 2, 16, 2, *block), bf16),
            pltpu.VMEM((32, *block), bf16),
            pltpu.VMEM((16, *block), bf16),
            pltpu.VMEM((15, *block), bf16),
            pltpu.VMEM((2, 256, 512), f32),
            pltpu.VMEM((2, 1024, 256), bf16),
            pltpu.VMEM((2, 64), i32),
            pltpu.SMEM((2, 64), i32),
            pltpu.VMEM((32, 2, 128), f32),
            pltpu.VMEM((16, 2, 2, 128), f32),
            pltpu.VMEM((15, 2, 2, 128), f32),
            pltpu.VMEM((8, 2, 128), f32),
            pltpu.VMEM((2, 128), f32),
            pltpu.SemaphoreType.REGULAR((2,)), dma((3,)), dma((8,)), dma((12,)), dma((8,)), dma((6,)), dma((5,)), dma((2,)), dma, dma,
            dma, dma, dma, dma, dma, dma, dma, dma,
        ],
        compiler_params=pltpu.CompilerParams(collective_id=0, has_side_effects=True, vmem_limit_bytes=55224 * 1024),
    )(pair_con, pair_val, screened, amplitude, qmap)


def solution(mesh):
    placed = (
        P("blk", None, None, "ga"),
        P("blk", None, None, "ga"),
        P("blk", None, "ga"),
        P("blk", None),
        P("blk", None),
    )
    return jax.shard_map(
        body, mesh=mesh, in_specs=placed, out_specs=P("blk", None), check_vma=False
    )
```

```python
import jax
import jax.numpy as jnp
from jax import lax
from jax.experimental import pallas as pl
from jax.experimental.pallas import tpu as pltpu
from jax.sharding import PartitionSpec as P

MESH = pl.DeviceIdType.MESH
ORDER = ((2, 2), (1, 1), (3, 3), (1, 3), (3, 1), (2, 1), (1, 2), (2, 3), (3, 2), (2, 0), (0, 2), (0, 3), (1, 0), (3, 0), (0, 1), (0, 0))
HERE = 15
GROUPS = ((0, 4), (4, 4), (8, 4), (12, 2), (14, 1), (15, 1))
Y_OF = (0, 0, 1, 1, 2, 2, 3, 3, 4, 4, 5, 5, 6, 7, 8, 9)
LO_OF = Y_OF[:14] + (11, 10)
PARTNER_OF = ((0, 0),) * 4 + ((1, 1),) * 4 + ((2, 2),) * 4 + ((3, 3),) * 2 + ((4, 7),) + ((5, 6),)


def group_of(t):
    return [t0 <= t < t0 + n for t0, n in GROUPS].index(True)


def iota(shape, dim):
    return lax.broadcasted_iota(jnp.int32, shape, dim)


def zero_one(cond):
    return jnp.where(cond, 1.0, 0.0).astype(jnp.bfloat16)


def kernel(
    con_hbm, val_hbm, w_hbm, amp_ref, qmap_hbm, out_ref,
    qmap_ref, con_raw, val_raw, w, s_send, d_send, vs_send, vd_send, con_all, val_all, transit, val_transit,
    acc, weight, rows_ref, partner, qa_all, part, gathered, fin, crossing,
    ready, load_sem, con_rs, y_rs, p_rs, val_rs, vt_rs, qa_rs, home_rs, fin_rs,
    con_ss, vd_ss, val_ss, relay_ss, d2d_ss, qa_ss, home_ss, fin_ss,
):
    blk, ga = lax.axis_index("blk"), lax.axis_index("ga")
    lo, x, z = blk // 16, (blk // 4) % 4, blk % 4
    h, c = ga // 2, ga % 2

    def dev(dx, dz, flip_lo=0, flip_h=0, flip_c=0):
        to_lo = (lo + flip_lo) % 2
        to_h = (h + flip_h) % 2
        to_c = (c + flip_c) % 2
        return (to_lo * 16 + ((x + dx + 4) % 4) * 4 + (z + dz + 4) % 4, to_h * 2 + to_c)

    loads = [
        pltpu.make_async_copy(con_hbm, con_raw, load_sem.at[0]),
        pltpu.make_async_copy(val_hbm, val_raw, load_sem.at[1]),
        pltpu.make_async_copy(w_hbm, w, load_sem.at[1]),
        pltpu.make_async_copy(qmap_hbm, qmap_ref, load_sem.at[2]),
    ]
    near = [(0, 0, 1, 0, 0), (0, 0, 1, 1, 0), (0, 0, 0, 0, 1), (1, 0, 0, 0, 0), (3, 0, 0, 0, 0), (0, 1, 0, 0, 0), (0, 3, 0, 0, 0)]
    along_x = [(d, 0, 0, 0, 0) for d in (2, 1, 3)]
    other_core = [(0, 0, 0, 0, 1)]
    barrier = pltpu.get_barrier_semaphore()
    for offset in near:
        pl.semaphore_signal(barrier, inc=1, device_id=dev(*offset), device_id_type=MESH)
    for n in (3, 1, 0):
        loads[n].start()

    def tell(stage, group):
        for offset in group:
            pl.semaphore_signal(ready.at[stage], inc=1, device_id=dev(*offset), device_id_type=MESH)

    def send(src, dst, ss, rs, to):
        pltpu.make_async_remote_copy(src, dst, ss, rs, device_id=to, device_id_type=MESH).start()

    def arrived(dst, rs):
        pltpu.make_async_copy(dst, dst, rs).wait()

    sent = arrived

    loads[3].wait()
    qmap = qmap_ref[...]
    for k in (0, 1):
        hit = qmap[k : k + 1, :] == iota((64, 64), 0)
        column = jnp.max(jnp.where(hit, iota((64, 64), 1), 0), axis=1, keepdims=True)
        square = jnp.where(iota((64, 64), 0) == iota((64, 64), 1), column, 0)
        rows_ref[k : k + 1, :] = jnp.max(square, axis=0, keepdims=True)
    to_smem = pltpu.make_async_copy(rows_ref, partner, load_sem.at[2])
    to_smem.start()
    place = zero_one(iota((16, 128), 0) + 64 == iota((16, 128), 1))
    moved = jnp.dot(amp_ref[...], place, preferred_element_type=jnp.float32)
    qa_all[blk] = moved + jnp.concatenate([qmap.astype(jnp.float32), jnp.zeros((2, 64), jnp.float32)], axis=1)
    to_smem.wait()

    def ordered(raw, k, q, dx, dz, fl):
        return raw[k, partner[k, dev(dx, dz, fl)[0] * 2 + q]]

    loads[1].wait()
    for fl, buffer in ((1, vd_send), (0, vs_send)):
        for t, (dx, dz) in enumerate(ORDER):
            for q in (0, 1):
                for k in (0, 1):
                    tile = ordered(val_raw, k, q, dx, dz, fl)
                    if t == HERE and not fl:
                        val_all[2 * HERE, q, k] = tile
                    else:
                        buffer[t, q, k] = tile
    pl.semaphore_wait(barrier, len(near))
    tell(0, near)

    def val_along_y(t):
        some = pl.ds(t, 3)
        send(vd_send.at[some], val_transit.at[some], vd_ss, vt_rs.at[t // 3], dev(0, 0, 1))

    def val_onward(t):
        some = pl.ds(t, 3)
        arrived(val_transit.at[some], vt_rs.at[t // 3])
        for u in range(t, t + 3):
            send(val_transit.at[u], val_all.at[2 * u + 1], val_ss, val_rs.at[group_of(u)], dev(*ORDER[u]))

    for t in range(0, 15, 3):
        val_along_y(t)
    loads[0].wait()
    for t, (dx, dz) in enumerate(ORDER):
        for fl, buffer in ((1, d_send), (0, s_send)):
            for q in (0, 1):
                for k in (0, 1):
                    tile = ordered(con_raw, k, q, dx, dz, fl)
                    if t != HERE:
                        buffer[t, q, k] = tile
                    elif fl:
                        transit[HERE, q, k] = tile
                    else:
                        con_all[0, 0, HERE, 0, q, k] = tile
    loads[2].start()
    pl.semaphore_wait(ready.at[0], len(near))
    tell(1, along_x + other_core)
    pl.semaphore_wait(ready.at[1], 4)
    for t in range(15):
        send(qa_all.at[blk], qa_all.at[blk], qa_ss, qa_rs.at[0], dev(*ORDER[t]))
    for block in range(0, 15, 4):
        for t in range(block, min(block + 4, 15)):
            send(d_send.at[t], transit.at[t], con_ss, con_rs.at[t // 2], dev(*ORDER[t]))
        for t in range(block, min(block + 4, 15)):
            send(s_send.at[t], con_all.at[0, 0, t, 0], con_ss, con_rs.at[t // 2], dev(*ORDER[t]))
    for t in range(15):
        send(vs_send.at[t], val_all.at[2 * t], val_ss, val_rs.at[group_of(t)], dev(*ORDER[t]))

    def relay(t):
        send(transit.at[t], con_all.at[0, 0, t, 1], relay_ss, y_rs.at[LO_OF[t]], dev(0, 0, 1))
        send(transit.at[t], con_all.at[0, 1, t, 1], relay_ss, y_rs.at[Y_OF[t]], dev(0, 0, 1, 1))
        send(con_all.at[0, 0, t, 0], con_all.at[0, 1, t, 0], relay_ss, y_rs.at[Y_OF[t]], dev(0, 0, 0, 1))

    def forward(t, n, gh):
        some = con_all.at[0, gh, pl.ds(t, n)]
        send(some, con_all.at[1, gh, pl.ds(t, n)], d2d_ss, p_rs.at[PARTNER_OF[t][gh]], dev(0, 0, 0, 0, 1))

    def come(t, n):
        arrived(val_all.at[pl.ds(0, 3 * n)], y_rs.at[Y_OF[t]])
        for gh in (0, 1):
            forward(t, n, gh)

    def weights():
        arrived(qa_all.at[pl.ds(0, 16)], qa_rs.at[1])
        table = qa_all[...].reshape(64, 128)
        amps = table.astype(jnp.bfloat16)
        pick = zero_one(iota((128, 128), 0) == iota((128, 128), 1) + 64)
        amps = jnp.dot(amps, pick, preferred_element_type=jnp.float32).astype(jnp.bfloat16)
        row = iota((64, 64), 0)
        source = jnp.zeros((64, 64), jnp.int32)
        for t, (dx, dz) in enumerate(ORDER):
            for fl in (0, 1):
                source = jnp.where(row // 2 == t * 2 + fl, dev(-dx, -dz, fl)[0] * 2, source)
        perm = zero_one(source + row % 2 == iota((64, 64), 1))
        for q in (0, 1):
            mine = (blk * 2 + q).astype(jnp.float32)
            hot = zero_one(table[:, :64] == mine)
            chosen = jnp.dot(hot, amps, preferred_element_type=jnp.float32).astype(jnp.bfloat16)
            chosen = jnp.dot(perm, chosen, preferred_element_type=jnp.float32).astype(jnp.bfloat16)
            spread = zero_one(iota((256, 16), 0) // 16 == iota((256, 16), 1))
            columns = zero_one((iota((128, 256), 0) // 4 == iota((128, 256), 1) % 4) & (iota((128, 256), 0) < 16))
            for t0, n in GROUPS:
                rows = jnp.dot(spread[: 64 * n, : 4 * n], chosen[4 * t0 : 4 * (t0 + n)], preferred_element_type=jnp.float32)
                rows = jnp.where(iota((64 * n, 128), 0) % 4 == iota((64 * n, 128), 1) % 4, rows, 0.0).astype(jnp.bfloat16)
                full = jnp.dot(rows, columns, preferred_element_type=jnp.float32)
                same = iota((64 * n, 256), 0) // 16 == iota((64 * n, 256), 1) // 16
                weight[q, 64 * t0 : 64 * (t0 + n)] = jnp.where(same, full, 0.0).astype(jnp.bfloat16)

    def quarter(t0, n, gc, gh, first=False):
        g = ((h + gh) % 2) * 2 + (c + gc) % 2

        def one(q, carry):
            lhs = con_all[gc, gh, t0 : t0 + n, :, q].reshape(64 * n, 512)
            rhs = w[q, pl.ds(pl.multiple_of(g * 512, 512), 512), :]
            product = jnp.dot(lhs, rhs, preferred_element_type=jnp.float32)
            if first:
                acc[q, : 64 * n] = product
            else:
                acc[q, : 64 * n] += product
            return carry

        lax.fori_loop(0, 2, one, 0)

    def own(t0, n):
        quarter(t0, n, 0, 0, True)
        quarter(t0, n, 0, 1)

    def others(t0, n):
        arrived(con_all.at[1, :, pl.ds(t0, n)], p_rs.at[PARTNER_OF[t0][0]])
        quarter(t0, n, 1, 0)
        quarter(t0, n, 1, 1)

    def terms(t0, n):
        first = 2 * t0 + (t0 == HERE)
        some = pl.ds(first, 2 * (t0 + n) - first)
        arrived(val_all.at[some], val_rs.at[group_of(t0)])
        size = 64 * n
        total = jnp.zeros((size, size), jnp.float32)
        for q in (0, 1):
            vals = val_all[2 * t0 : 2 * (t0 + n), q].reshape(size, 512)
            unit = acc[q, :size].astype(jnp.bfloat16)
            full = lax.dot_general(unit, vals, (((1,), (1,)), ((), ())), preferred_element_type=jnp.float32)
            total = total + full * weight[q, 64 * t0 : 64 * (t0 + n), :size].astype(jnp.float32)
        lanes = iota((size, 128), 1)
        columns = zero_one(((iota((size, 128), 0) // 4) % 4 == lanes // 4) & (lanes < 16))
        high = total.astype(jnp.bfloat16)
        low = (total - high.astype(jnp.float32)).astype(jnp.bfloat16)
        summed = jnp.dot(high, columns, preferred_element_type=jnp.float32)
        summed = summed + jnp.dot(low, columns, preferred_element_type=jnp.float32)
        summed = jnp.where((iota((size, 128), 0) // 4) % 4 == lanes % 4, summed, 0.0)
        part[t0 : t0 + n] = jnp.sum(summed.reshape(4 * n, 16, 128), axis=1).reshape(n, 2, 2, 128)

    def home(t0, n):
        for t in range(t0, t0 + n):
            dx, dz = ORDER[t]
            send(part.at[t], gathered.at[t], home_ss, home_rs, dev(-dx, -dz))

    for t in range(15):
        if t % 2 == 0:
            n = min(2, 15 - t)
            arrived(con_all.at[0, 0, pl.ds(t, n)], con_rs.at[t // 2])
        relay(t)
        if t == 3:
            arrived(qa_all.at[pl.ds(0, 15)], qa_rs.at[0])
            plane = qa_all.at[pl.ds(lo * 16, 16)]
            send(plane, plane, qa_ss, qa_rs.at[1], dev(0, 0, 1))
        if t % 3 == 2:
            val_onward(t - 2)
    weights()
    loads[2].wait()
    for t in range(0, 14, 2):
        if t < 12:
            come(t, 2)
        else:
            come(12, 1)
        if t in (4, 8, 12):
            others(t - 4, 4)
            terms(t - 4, 4)
            home(t - 4, 4)
        if t in (2, 6, 10):
            own(t - 2, 4)
    come(13, 1)
    relay(HERE)
    send(vd_send.at[HERE], val_all.at[2 * HERE + 1], vd_ss, val_rs.at[group_of(HERE)], dev(0, 0, 1))
    own(12, 2)
    others(12, 2)
    terms(12, 2)
    home(12, 2)
    for t in (14, HERE):
        arrived(con_all.at[0, 0, t, 1], y_rs.at[LO_OF[t]])
        forward(t, 1, 0)
        quarter(t, 1, 0, 0, True)
        arrived(con_all.at[0, 1, t], y_rs.at[Y_OF[t]])
        forward(t, 1, 1)
        quarter(t, 1, 0, 1)
        arrived(con_all.at[1, 0, t], p_rs.at[PARTNER_OF[t][0]])
        quarter(t, 1, 1, 0)
        arrived(con_all.at[1, 1, t], p_rs.at[PARTNER_OF[t][1]])
        quarter(t, 1, 1, 1)
        if t == 14:
            terms(14, 1)
            home(14, 1)
    terms(HERE, 1)
    arrived(gathered, home_rs)
    column = part[HERE] + jnp.sum(gathered[...], axis=0)
    fin[ga] = column[0]
    crossing[...] = column[1]
    for gh, gc in ((1, 0), (1, 1), (0, 1)):
        send(fin.at[ga], fin.at[ga], fin_ss, fin_rs, dev(0, 0, 0, gh, gc))
    for gh, gc in ((1, 0), (1, 1), (0, 0), (0, 1)):
        send(crossing, fin.at[4 + ga], fin_ss, fin_rs, dev(0, 0, 1, gh, gc))
    arrived(fin.at[pl.ds(1, 7)], fin_rs)
    out_ref[...] = jnp.sum(fin[...], axis=0)[:, :16] / 64.0

    sent(val_all.at[pl.ds(0, 30)], con_ss)
    sent(con_all.at[0, :, pl.ds(0, 12)], relay_ss)
    sent(con_all.at[0], d2d_ss)
    sent(vd_send, vd_ss)
    sent(val_all.at[pl.ds(0, 30)], val_ss)
    sent(qa_all.at[pl.ds(0, 31)], qa_ss)
    sent(gathered, home_ss)
    sent(fin.at[pl.ds(1, 7)], fin_ss)


def body(pair_val, pair_con, screened, amplitude, qmap):
    bf16, f32, i32 = jnp.bfloat16, jnp.float32, jnp.int32
    block = (2, 2, 16, 512)
    dma = pltpu.SemaphoreType.DMA
    hbm = pl.BlockSpec(memory_space=pl.ANY)
    vmem = pl.BlockSpec(memory_space=pltpu.VMEM)
    return pl.pallas_call(
        kernel,
        out_shape=jax.ShapeDtypeStruct((2, 16), f32),
        in_specs=[hbm, hbm, hbm, vmem, hbm],
        out_specs=vmem,
        scratch_shapes=[
            pltpu.VMEM((2, 64), i32),
            pltpu.VMEM((2, 64, 16, 512), bf16),
            pltpu.VMEM((2, 64, 16, 512), bf16),
            pltpu.VMEM((2, 2048, 512), bf16),
            pltpu.VMEM((15, *block), bf16),
            pltpu.VMEM((15, *block), bf16),
            pltpu.VMEM((15, *block), bf16),
            pltpu.VMEM((16, *block), bf16),
            pltpu.VMEM((2, 2, 16, 2, *block), bf16),
            pltpu.VMEM((32, *block), bf16),
            pltpu.VMEM((16, *block), bf16),
            pltpu.VMEM((15, *block), bf16),
            pltpu.VMEM((2, 256, 512), f32),
            pltpu.VMEM((2, 1024, 256), bf16),
            pltpu.VMEM((2, 64), i32),
            pltpu.SMEM((2, 64), i32),
            pltpu.VMEM((32, 2, 128), f32),
            pltpu.VMEM((16, 2, 2, 128), f32),
            pltpu.VMEM((15, 2, 2, 128), f32),
            pltpu.VMEM((8, 2, 128), f32),
            pltpu.VMEM((2, 128), f32),
            pltpu.SemaphoreType.REGULAR((2,)), dma((3,)), dma((8,)), dma((12,)), dma((8,)), dma((6,)), dma((5,)), dma((2,)), dma, dma,
            dma, dma, dma, dma, dma, dma, dma, dma,
        ],
        compiler_params=pltpu.CompilerParams(collective_id=0, has_side_effects=True, vmem_limit_bytes=55224 * 1024),
    )(pair_con, pair_val, screened, amplitude, qmap)


def solution(mesh):
    placed = (
        P("blk", None, None, "ga"),
        P("blk", None, None, "ga"),
        P("blk", None, "ga"),
        P("blk", None),
        P("blk", None),
    )
    return jax.shard_map(
        body, mesh=mesh, in_specs=placed, out_specs=P("blk", None), check_vma=False
    )
```
